512 devices in a mesh: row: 16 (over x, y_hi, core), col: 32 (over y_lo, z).
Axes of the slice: x: 4, y: 8 (y_hi: 2, y_lo: 4; y = y_hi * 4 + y_lo), z: 8, core: 2. Of those that a mesh axis runs over, the one named last changes fastest.
Arguments:
- resident: float32 [12288, 12288], P('row', 'col')
- factor: float32 [1, 12288, 512], P(None, 'col', 'row'), may hold values from -0.078125 to 0.078125
- dinv: float32 [1, 512, 512], P(None, 'col')
- panel_cols: int32 [1, 512], replicated, may hold values from 0 to 12287, as said below
- row_lists: int32 [1, 6144], replicated, may hold values from 0 to 12287, as said below
Outputs:
- inverse_out: float32 [12288, 12288], P('row', 'col')
The draws below stay inside these ranges and needn't reach their ends.
Inputs may be any that keep to these rules, and one draw needn't show every extreme that they name: The entries of panel_cols are distinct positions. The resident array and every dinv[k] are symmetric. Each row_lists[k] holds distinct positions, none of them in panel_cols[j] for any j <= k.
All inputs are finite; a program needn't handle non-finite values.
Results may differ from the reference program's by a relative error of at most 0.0001.
Values sent between devices are 32-bit elements; how exact they have to be, the bound alone decides.
No kernel may reach another device: no remote copies, remote signals or barrier semaphores. Data moves between devices by JAX's collectives and lax.ppermute only.
A program may use at most 64 MiB of HBM per device.

```python
import jax
import jax.numpy as jnp
from jax import lax

N = 12288
PW = 512
PANELS = 1
SROWS = 6144


def index_sets(key):
    order = jax.random.permutation(jax.random.fold_in(key, 7), N).astype(jnp.int32)
    columns = order[:PANELS * PW].reshape(PANELS, PW)
    picks = []
    for panel in range(PANELS):
        remain = order[(panel + 1) * PW:]
        shuffled = jax.random.permutation(jax.random.fold_in(key, 11 + panel), remain)
        picks.append(shuffled[:SROWS])
    return (columns, jnp.stack(picks).astype(jnp.int32))


def draw_panel_cols(key, part):
    return index_sets(key)[0]


def draw_row_lists(key, part):
    return index_sets(key)[1]


def draw_resident(key, part):
    base = jax.random.normal(jax.random.fold_in(key, 3), (N, N), jnp.float32)
    sym = (base + base.T) * 0.7071
    return sym + 2.0 * jnp.eye(N, dtype=jnp.float32)


def draw_dinv(key, part):
    base = jax.random.normal(jax.random.fold_in(key, 13), (PANELS, PW, PW), jnp.float32)
    sym = (base + jnp.swapaxes(base, 1, 2)) * 0.5
    return sym + 1.5 * jnp.eye(PW, dtype=jnp.float32)[None]


def shard_levels(key, dims, cuts, least, largest):
    level, own = 1.0, jax.random.fold_in(key, 6)
    for dim, blocks in cuts:
        draws = jnp.exp(jax.random.uniform(jax.random.fold_in(own, dim), (blocks,), jnp.float32, least / len(cuts), largest / len(cuts)))
        level = level * jnp.repeat(draws, dims[dim] // blocks).reshape([-1 if axis == dim else 1 for axis in range(len(dims))])
    return level


def gaussian(stream_key, extent, spread, reach, split=(), kind=jnp.bfloat16):
    loudness = shard_levels(stream_key, extent, split, -0.22, 0.18) if split else 1.0
    result = jax.random.normal(stream_key, extent, jnp.float32) * spread * loudness
    return jnp.minimum(jnp.maximum(result, -reach), reach).astype(kind)


def setup_inputs(seed: int = 0) -> dict:
    key_of = jax.random.split(jax.random.key(seed), 6)
    return {
        "resident": draw_resident(jax.random.fold_in(key_of[5], 71), 0),
        "factor": gaussian(key_of[1], (PANELS, N, PW), SROWS ** -0.5, 0.078125, ((1, 32), (2, 16)), jnp.float32),
        "dinv": draw_dinv(jax.random.fold_in(key_of[5], 71), 0),
        "panel_cols": draw_panel_cols(jax.random.fold_in(key_of[5], 71), 0),
        "row_lists": draw_row_lists(jax.random.fold_in(key_of[5], 71), 0),
    }


def reference(resident, factor, dinv, panel_cols, row_lists):
    highest = lax.Precision.HIGHEST
    matrix = resident
    for panel in reversed(range(PANELS)):
        rows = row_lists[panel].astype(jnp.int32)
        cols = panel_cols[panel].astype(jnp.int32)
        lower = jnp.zeros((N, PW), jnp.float32).at[rows].set(factor[panel][rows])
        product = -jnp.dot(matrix, lower, precision=highest)
        picked = product[rows]
        gram_block = jnp.dot(lower.T, product, precision=highest)
        matrix = matrix.at[rows[:, None], cols[None, :]].set(picked)
        matrix = matrix.at[cols[:, None], rows[None, :]].set(picked.T)
        matrix = matrix.at[cols[:, None], cols[None, :]].set(dinv[panel] - gram_block)
    return matrix
```

```python
import jax
import jax.numpy as jnp
from jax import lax
from jax.sharding import Mesh
from jax.sharding import PartitionSpec as P

ROW = ("row_0", "row_1", "row_2")
HIGHEST = lax.Precision.HIGHEST


def split_up(shard, dim, count):
    shape = shard.shape
    blocks = shard.reshape(*shape[:dim], count, shape[dim] // count, *shape[dim + 1 :])
    return jnp.moveaxis(blocks, dim, 0)


def sum_at_owner(shard, axis, dim):
    count = lax.axis_size(axis)
    blocks = lax.all_to_all(split_up(shard, dim, count), axis, 0, 0, tiled=True)
    return jnp.sum(blocks, axis=0)


def sent_to_all(shard, axis):
    copies = jnp.broadcast_to(shard, (lax.axis_size(axis), *shard.shape))
    return lax.all_to_all(copies, axis, split_axis=0, concat_axis=0, tiled=True)


def ring_sum(shard, axis):
    count = lax.axis_size(axis)
    ring = [(place, (place + 1) % count) for place in range(count)]

    def step(_, carried):
        moving, total = carried
        moving = lax.ppermute(moving, axis, ring)
        return moving, total + moving

    return lax.fori_loop(0, count - 1, step, (shard, shard))[1]


def general_panel(matrix, factor, dinv, panel_cols, row_lists):
    row_count = lax.axis_size(ROW)
    col_count = lax.axis_size("col")
    ratio = col_count // row_count
    row_block, col_block = matrix.shape
    total = row_block * row_count
    width = panel_cols.shape[0]
    dinv_rows = dinv.shape[0]
    row_pos = lax.axis_index(ROW)
    col_pos = lax.axis_index("col")
    row_ids = row_pos * row_block + jnp.arange(row_block, dtype=jnp.int32)
    col_ids = col_pos * col_block + jnp.arange(col_block, dtype=jnp.int32)
    in_rows = jnp.zeros((total,), jnp.float32).at[row_lists].set(1.0)
    panel_map = (
        jnp.full((total,), -1, jnp.int32)
        .at[panel_cols]
        .set(jnp.arange(width, dtype=jnp.int32))
    )
    col_mask = in_rows[col_ids]
    part_width = factor.shape[1]
    own_part = lax.dynamic_update_slice(
        jnp.zeros((col_block, width), jnp.float32), factor, (0, row_pos * part_width)
    )
    lower_cols = ring_sum(own_part, ROW) * col_mask[:, None]
    product_rows = ring_sum(-jnp.dot(matrix, lower_cols, precision=HIGHEST), "col")
    owner = col_pos // ratio
    offset = col_pos % ratio * col_block
    mine = lax.dynamic_slice_in_dim(product_rows, offset, col_block, 0)
    masked = jnp.where(row_pos == owner, mine, jnp.zeros_like(mine))
    product_cols = ring_sum(masked, ROW)
    placed = lax.dynamic_update_slice(
        jnp.zeros((width, width), jnp.float32), dinv, (col_pos * dinv_rows, 0)
    )
    gram_term = jnp.dot(lower_cols.T, product_cols, precision=HIGHEST)
    diagonal = ring_sum(placed - gram_term, "col")
    row_slot = panel_map[row_ids]
    col_slot = panel_map[col_ids]
    row_safe = jnp.maximum(row_slot, 0)
    col_safe = jnp.maximum(col_slot, 0)
    row_in = in_rows[row_ids] > 0.5
    col_in = col_mask > 0.5
    row_panel = row_slot >= 0
    col_panel = col_slot >= 0
    below = jnp.take(product_rows, col_safe, axis=1)
    beside = jnp.take(product_cols, row_safe, axis=1).T
    corner = jnp.take(jnp.take(diagonal, row_safe, axis=0), col_safe, axis=1)
    return jnp.where(
        row_panel[:, None] & col_panel[None, :],
        corner,
        jnp.where(
            row_panel[:, None] & col_in[None, :],
            beside,
            jnp.where(row_in[:, None] & col_panel[None, :], below, matrix),
        ),
    )


def dot(a, b, dims=((1,), (0,))):
    return lax.dot_general(
        a, b, (dims, ((), ())), precision=HIGHEST, preferred_element_type=jnp.float32
    )


def places(ids, base, listed):
    member = jnp.any(ids[:, None] == listed[None, :], axis=1)
    between = (listed[None, :] < ids[:, None]) & (listed[None, :] >= base[:, None])
    return member, jnp.sum(between.astype(jnp.int32), axis=1)


def one_hot(member, slot, count):
    return ((slot[:, None] == jnp.arange(count)) & member[:, None]).astype(jnp.float32)


def packed_panel(row_slots, col_slots, matrix, factor, dinv, panel_cols, row_lists):
    row_count = lax.axis_size(ROW)
    col_count = lax.axis_size("col")
    ratio = col_count // row_count
    row_block, col_block = matrix.shape
    width = panel_cols.shape[0]
    dinv_rows = dinv.shape[0]
    row_pos = lax.axis_index(ROW)
    col_pos = lax.axis_index("col")
    far, across, core = (lax.axis_index(axis) for axis in ROW)

    blocks = jnp.stack([col_pos] + [row_pos * ratio + part for part in range(ratio)])
    ids = (blocks[:, None] * col_block + jnp.arange(col_block, dtype=jnp.int32)).reshape(-1)
    base = jnp.repeat(blocks * col_block, col_block)
    in_list, list_slot = places(ids, base, row_lists)
    in_panel, panel_slot = places(ids, base, panel_cols)
    col_in, row_in = in_list[:col_block], in_list[col_block:]
    col_panel, row_panel = in_panel[:col_block], in_panel[col_block:]
    pick = one_hot(in_list, list_slot, row_slots)
    pick_cols = pick[:col_block]
    pick_rows = pick[col_block:].reshape(ratio, col_block, row_slots)
    put = one_hot(in_panel, panel_slot, col_slots)
    put_cols = put[:col_block]

    packed = dot(factor, pick_cols, ((0,), (0,)))
    swap = [(0, 1), (1, 0)]
    other = lax.ppermute(packed, "row_1", swap)
    pair = jnp.stack(
        [jnp.where(across == 0, packed, other), jnp.where(across == 0, other, packed)]
    )
    own_half = sent_to_all(pair, "row_0").reshape(width // 2, row_slots)
    other_half = lax.ppermute(own_half, "row_2", swap)
    lower = jnp.concatenate([own_half, other_half])

    narrow = dot(matrix, pick_cols).reshape(ratio, col_block, row_slots)
    dense = jnp.concatenate(
        [dot(pick_rows[part], narrow[part], ((0,), (0,))) for part in range(ratio)]
    )

    home = panel_cols // col_block
    earlier = (panel_cols[None, :] < panel_cols[:, None]) & (home[None, :] == home[:, None])
    slot = home * col_slots + jnp.sum(earlier.astype(jnp.int32), axis=1)
    by_core = jnp.moveaxis(slot.reshape(-1, 2, factor.shape[1]), 1, 0).reshape(2, width // 2)
    local = jnp.where(core == 0, by_core, by_core[::-1]).reshape(width)
    slots = jnp.arange(col_count * col_slots, dtype=jnp.int32)
    route = (local[:, None] == slots).astype(jnp.float32)
    row_k = ratio * col_slots
    route_rows = (slot[:, None] - row_pos * row_k == jnp.arange(row_k)).astype(jnp.float32)
    mine = lax.dynamic_slice_in_dim(slot, col_pos * dinv_rows, dinv_rows)
    route_mine = (mine[:, None] == slots).astype(jnp.float32)
    placed = dot(route_mine, dot(dinv, route_rows), ((0,), (0,)))
    lower_slots = dot(route, lower, ((0,), (0,)))

    partial_value = -dot(dense, lower, ((1,), (1,)))
    summed = sum_at_owner(partial_value, "col", 0)

    chosen = dot(summed, route)
    parts = split_up(chosen, 1, col_count)
    arrived = lax.all_to_all(parts, "col", 0, 0, tiled=True)
    below = arrived.reshape(-1, col_slots)

    halves = jnp.moveaxis(below.reshape(ratio, row_slots, col_slots), 1, 2)
    sides = []
    for turn in range(ratio):
        pairs = [
            (r * col_count + c, (c // ratio) * col_count + ratio * r + (c + turn) % ratio)
            for r in range(row_count)
            for c in range(col_count)
        ]
        part = lax.dynamic_index_in_dim(halves, (col_pos + turn) % ratio, 0, False)
        sides.append(lax.ppermute(part, ROW + ("col",), pairs))
    sides = jnp.stack(sides)
    order = (col_pos - jnp.arange(ratio)) % ratio
    turned = jnp.stack(
        [lax.dynamic_index_in_dim(sides, order[part], 0, False) for part in range(ratio)]
    )
    beside = turned.reshape(row_k, row_slots)

    gram = dot(lower_slots, beside, ((1,), (1,)))
    corner = sum_at_owner(placed - gram, "col", 0)

    put_rows = put[col_block:].reshape(ratio, col_block, col_slots)
    below_rows = jnp.concatenate(
        [
            dot(pick_rows[part], below[part * row_slots : (part + 1) * row_slots])
            for part in range(ratio)
        ]
    )
    corner_rows = jnp.concatenate(
        [
            dot(put_rows[part], corner[:, part * col_slots : (part + 1) * col_slots], ((1,), (1,)))
            for part in range(ratio)
        ]
    )
    at_cols = dot(below_rows + corner_rows, put_cols, ((1,), (1,)))
    wide = dot(beside, pick_cols, ((1,), (1,)))
    at_rows = jnp.concatenate(
        [
            dot(put_rows[part], wide[part * col_slots : (part + 1) * col_slots])
            for part in range(ratio)
        ]
    )
    return jnp.where(
        (row_panel | row_in)[:, None] & col_panel[None, :],
        at_cols,
        jnp.where(row_panel[:, None] & col_in[None, :], at_rows, matrix),
    )


def fullest(listed, col_block, col_count):
    home = listed // col_block
    counts = jnp.sum((home[:, None] == jnp.arange(col_count)).astype(jnp.int32), axis=0)
    return jnp.max(counts)


def on_device(resident, factor, dinv, panel_cols, row_lists):
    col_count = lax.axis_size("col")
    col_block = resident.shape[1]
    row_slots = col_block * 2 // 3
    col_slots = 2 * (panel_cols.shape[1] // col_count)
    matrix = resident
    for panel in reversed(range(factor.shape[0])):
        fits = (fullest(row_lists[panel], col_block, col_count) <= row_slots) & (
            fullest(panel_cols[panel], col_block, col_count) <= col_slots
        )
        matrix = lax.cond(
            fits,
            lambda *args: packed_panel(row_slots, col_slots, *args),
            general_panel,
            matrix,
            factor[panel],
            dinv[panel],
            panel_cols[panel],
            row_lists[panel],
        )
    return matrix


def solution(mesh):
    finer = Mesh(
        mesh.devices.reshape(-1, 2, 2, mesh.shape["col"]), ("row_0", "row_1", "row_2", "col")
    )
    return jax.shard_map(
        on_device,
        mesh=finer,
        in_specs=(P(ROW, "col"), P(None, "col", ROW), P(None, "col", None), P(), P()),
        out_specs=P(ROW, "col"),
        check_vma=False,
    )
```

```python
import functools

import jax
import jax.numpy as jnp
from jax import lax
from jax.experimental import pallas as pl
from jax.experimental.pallas import tpu as pltpu
from jax.sharding import Mesh
from jax.sharding import PartitionSpec as P

ROW = ("row_0", "row_1", "row_2")
HIGHEST = lax.Precision.HIGHEST
LANES = 128
LINES = 16
BY_LAST = ((1,), (1,))
BY_FIRST = ((0,), (0,))


def dot(a, b, dims=((1,), (0,))):
    return lax.dot_general(
        a, b, (dims, ((), ())), precision=HIGHEST, preferred_element_type=jnp.float32
    )


def sum_at_owner(blocks, axis):
    return jnp.sum(lax.all_to_all(blocks, axis, 0, 0, tiled=True), axis=0)


def sent_to_all(shard, axis):
    copies = jnp.broadcast_to(shard, (lax.axis_size(axis), *shard.shape))
    return lax.all_to_all(copies, axis, split_axis=0, concat_axis=0, tiled=True)


def ring_sum(shard, axis):
    count = lax.axis_size(axis)
    ring = [(place, (place + 1) % count) for place in range(count)]

    def step(_, carried):
        moving, total = carried
        moving = lax.ppermute(moving, axis, ring)
        return moving, total + moving

    return lax.fori_loop(0, count - 1, step, (shard, shard))[1]


def general_panel(matrix, factor, dinv, panel_cols, row_in, col_in):
    row_count = lax.axis_size(ROW)
    ratio = lax.axis_size("col") // row_count
    row_block, col_block = matrix.shape
    width = panel_cols.shape[0]
    group = factor.shape[1]
    row_pos = lax.axis_index(ROW)
    col_pos = lax.axis_index("col")
    row_ids = row_pos * row_block + jnp.arange(row_block, dtype=jnp.int32)
    col_ids = col_pos * col_block + jnp.arange(col_block, dtype=jnp.int32)
    masked = factor * col_in[:, None].astype(jnp.float32)

    def column_places(turn):
        cols = lax.dynamic_slice_in_dim(panel_cols, turn * group, group)
        return cols, (cols[:, None] == col_ids).astype(jnp.float32)

    def products(turn, carried):
        out, gram = carried
        lower = ring_sum(jnp.where(row_pos == turn, masked, jnp.zeros_like(masked)), ROW)
        by_row = ring_sum(-dot(matrix, lower), "col")
        mine = lax.dynamic_slice_in_dim(by_row, col_pos % ratio * col_block, col_block, 0)
        mine = jnp.where(row_pos == col_pos // ratio, mine, jnp.zeros_like(mine))
        by_col = ring_sum(mine, ROW)
        gram = lax.dynamic_update_slice(
            gram, dot(masked, by_col, BY_FIRST), (row_pos * group, turn * group)
        )
        cols, put_cols = column_places(turn)
        put_rows = (row_ids[:, None] == cols).astype(jnp.float32)
        here = jnp.sum(put_cols, axis=0) > 0.5
        there = jnp.sum(put_rows, axis=1) > 0.5
        out = jnp.where(
            row_in[:, None] & here[None, :],
            dot(by_row, put_cols),
            jnp.where(there[:, None] & col_in[None, :], dot(put_rows, by_col, BY_LAST), out),
        )
        return out, gram

    none = jnp.zeros((width, width), jnp.float32)
    out, gram = lax.fori_loop(0, row_count, products, (matrix, none))
    placed = lax.dynamic_update_slice(none, dinv, (col_pos * dinv.shape[0], 0))
    placed = jnp.where(row_pos == 0, placed, none)
    diagonal = ring_sum(ring_sum(placed - gram, ROW), "col")
    put_rows = (row_ids[:, None] == panel_cols).astype(jnp.float32)
    there = jnp.sum(put_rows, axis=1) > 0.5

    def corners(turn, out):
        _, put_cols = column_places(turn)
        here = jnp.sum(put_cols, axis=0) > 0.5
        part = lax.dynamic_slice_in_dim(diagonal, turn * group, group, 1)
        corner = dot(dot(put_rows, part), put_cols)
        return jnp.where(there[:, None] & here[None, :], corner, out)

    return lax.fori_loop(0, row_count, corners, out)


def slots_kernel(lines, lanes, device_ref, rows_ref, cols_ref, row_slots_ref, col_slots_ref):
    line = lax.broadcasted_iota(jnp.int32, (LINES, 1), 0)
    own = jnp.where(
        line < lines, device_ref[0] * lines + line, device_ref[1] * lines + line - lines
    )
    lower = lax.broadcasted_iota(jnp.int32, (lanes, lanes), 0)
    upper = lax.broadcasted_iota(jnp.int32, (lanes, lanes), 1)
    earlier = (lower < upper).astype(jnp.float32)
    for listed_ref, out_ref in ((rows_ref, row_slots_ref), (cols_ref, col_slots_ref)):
        count = listed_ref.shape[1]
        step = min(count, 1024)
        found = jnp.zeros((LINES, lanes), jnp.float32)
        for start in range(0, count, step):
            size = min(step, count - start)
            listed = listed_ref[:, start : start + size]
            high = lax.div(listed, jnp.int32(lanes))
            low = listed - high * lanes
            line_hit = (own == high).astype(jnp.float32)
            lane_hit = lax.broadcasted_iota(jnp.int32, (lanes, size), 0) == low
            found += lax.dot_general(
                line_hit.astype(jnp.bfloat16),
                lane_hit.astype(jnp.float32).astype(jnp.bfloat16),
                (BY_LAST, ((), ())),
                preferred_element_type=jnp.float32,
            )
        before = jnp.dot(
            found.astype(jnp.bfloat16),
            earlier.astype(jnp.bfloat16),
            preferred_element_type=jnp.float32,
        )
        held = jnp.sum(found, axis=1, keepdims=True)
        for other in range(LINES):
            if (other + 1) % lines:
                later = (line > other) & (line < (other // lines + 1) * lines)
                before += jnp.where(later, held[other : other + 1], 0.0)
        out_ref[...] = jnp.where(found > 0.5, before, -1.0).astype(jnp.int32)


def block_slots(col_block, ratio, panel_cols, row_lists):
    lanes = LANES if col_block % LANES == 0 else col_block
    lines = col_block // lanes
    device = jnp.stack([lax.axis_index("col"), lax.axis_index(ROW) * ratio]).astype(jnp.int32)
    shape = jax.ShapeDtypeStruct((LINES, lanes), jnp.int32)
    whole = pl.BlockSpec(memory_space=pltpu.VMEM)
    found = pl.pallas_call(
        functools.partial(slots_kernel, lines, lanes),
        out_shape=(shape, shape),
        in_specs=[pl.BlockSpec(memory_space=pltpu.SMEM), whole, whole],
        out_specs=(whole, whole),
        name="block_slots",
    )(device, row_lists[None], panel_cols[None])
    used = (1 + ratio) * lines
    return [slots[:used].reshape(used * lanes) for slots in found]


def one_hot(slot, count):
    return (slot[:, None] == jnp.arange(count, dtype=jnp.int32)).astype(jnp.float32)


def fullest(listed, col_block, col_count):
    home = listed // col_block
    counts = jnp.sum((jnp.arange(col_count)[:, None] == home).astype(jnp.int32), axis=1)
    return jnp.max(counts)


def panel_step(matrix, factor, dinv, panel_cols, row_lists):
    row_count = lax.axis_size(ROW)
    col_count = lax.axis_size("col")
    ratio = col_count // row_count
    row_block, col_block = matrix.shape
    width = panel_cols.shape[0]
    dinv_rows = dinv.shape[0]
    row_slots = col_block * 2 // 3
    col_slots = 2 * (width // col_count)
    row_k = ratio * col_slots
    row_pos = lax.axis_index(ROW)
    col_pos = lax.axis_index("col")
    side = col_pos % ratio

    list_slot, panel_slot = block_slots(col_block, ratio, panel_cols, row_lists)
    in_list, in_panel = list_slot >= 0, panel_slot >= 0
    col_in, row_in = in_list[:col_block], in_list[col_block:]
    col_panel, row_panel = in_panel[:col_block], in_panel[col_block:]
    pick = one_hot(list_slot, row_slots)
    pick_cols = pick[:col_block]
    pick_rows = pick[col_block:].reshape(ratio, col_block, row_slots)
    put = one_hot(panel_slot, col_slots)
    put_cols = put[:col_block]
    put_rows = put[col_block:].reshape(ratio, col_block, col_slots)

    packed = dot(factor, pick_cols, BY_FIRST)
    own_half = sent_to_all(packed, ROW[:2]).reshape(width // 2, row_slots)
    other_half = lax.ppermute(own_half, ROW[2], [(0, 1), (1, 0)])
    lower = jnp.concatenate([own_half, other_half])

    narrow = dot(matrix, pick_cols).reshape(ratio, col_block, row_slots)
    dense = jnp.stack([dot(pick_rows[part], narrow[part], BY_FIRST) for part in range(ratio)])
    share = row_slots // col_count
    dense = jnp.moveaxis(dense.reshape(ratio, col_count, share, row_slots), 0, 1)
    dense = dense.reshape(ratio * row_slots, row_slots)

    partial_value = -dot(dense, lower, BY_LAST)
    summed = sum_at_owner(partial_value.reshape(col_count, ratio * share, width), "col")

    home = panel_cols // col_block
    earlier = (panel_cols[None, :] < panel_cols[:, None]) & (home[None, :] == home[:, None])
    rank = jnp.sum(earlier.astype(jnp.int32), axis=1)
    slot = home * col_slots + rank
    wide = max(row_k, LANES)
    spread = home // ratio * wide + home % ratio * col_slots + rank
    half_slots = col_slots // 2

    def this_core_first(values):
        by_core = jnp.moveaxis(values.reshape(-1, 2, factor.shape[1]), 1, 0)
        by_core = by_core.reshape(2, width // 2)
        return jnp.where(lax.axis_index(ROW[2]) == 0, by_core, by_core[::-1]).reshape(width)

    route = one_hot(this_core_first(spread), row_count * wide)

    chosen = dot(summed, route).reshape(ratio, share, row_count, wide)
    chosen = jnp.transpose(chosen, (2, 0, 1, 3)).reshape(col_count, share, wide)
    arrived = lax.all_to_all(chosen, "col", 0, 0, tiled=True).reshape(row_slots, wide)
    arrived = arrived.T[:row_k]

    pairs = [
        (r * col_count + c, (c // ratio) * col_count + ratio * r + c % ratio)
        for r in range(row_count)
        for c in range(col_count)
    ]
    beside = lax.ppermute(arrived, ROW + ("col",), pairs)

    def halves(values):
        blocks = values.reshape(col_count, 2, half_slots, values.shape[1])
        return [blocks[:, part].reshape(col_count * half_slots, -1) for part in range(2)]

    slots = col_count * col_slots
    lower_slots = dot(one_hot(this_core_first(slot), slots), lower, BY_FIRST)
    mine = lax.dynamic_slice_in_dim(slot, col_pos * dinv_rows, dinv_rows)
    placed = dot(
        one_hot(mine, slots), dot(dinv, one_hot(slot - row_pos * row_k, row_k)), BY_FIRST
    )
    lower_pair = jnp.concatenate(halves(lower_slots), axis=1)
    placed_pair = jnp.concatenate(halves(placed), axis=1)
    empty = jnp.zeros_like(beside)
    beside_pair = jnp.concatenate(
        [jnp.concatenate([beside, empty], axis=1), jnp.concatenate([empty, beside], axis=1)]
    )
    terms = placed_pair - dot(lower_pair, beside_pair, BY_LAST)
    corner = sum_at_owner(terms.reshape(col_count, half_slots, 2 * row_k), "col")

    swap = [(c, c + 1 - 2 * (c % ratio)) for c in range(col_count)]
    kept = lax.dynamic_slice_in_dim(arrived, side * col_slots, col_slots, 0)
    given = lax.dynamic_slice_in_dim(arrived, (1 - side) * col_slots, col_slots, 0)
    taken = lax.ppermute(given, "col", swap)
    below = [jnp.where(side == 0, kept, taken), jnp.where(side == 0, taken, kept)]

    below_rows = [dot(pick_rows[part], below[part], BY_LAST) for part in range(ratio)]
    spread_out = dot(beside, pick_cols, BY_LAST)
    at_rows = jnp.concatenate(
        [
            dot(put_rows[part], spread_out[part * col_slots : (part + 1) * col_slots])
            for part in range(ratio)
        ]
    )
    with_rows = jnp.where(row_panel[:, None] & col_in[None, :], at_rows, matrix)
    at_cols = jnp.concatenate(
        [
            below_rows[part]
            + jnp.concatenate(
                [
                    dot(
                        put_rows[part],
                        corner[:, (half * ratio + part) * col_slots :][:, :col_slots],
                        BY_LAST,
                    )
                    for half in range(2)
                ],
                axis=1,
            )
            for part in range(ratio)
        ]
    )
    taken_over = (row_panel | row_in)[:, None] & col_panel[None, :]
    result = jnp.where(taken_over, dot(at_cols, put_cols, BY_LAST), with_rows)

    fits = (fullest(row_lists, col_block, col_count) <= row_slots) & (
        fullest(panel_cols, col_block, col_count) <= col_slots
    )

    def again(carried):
        general = general_panel(matrix, factor, dinv, panel_cols, row_in, col_in)
        return jnp.zeros((), jnp.bool_), general

    return lax.while_loop(lambda carried: carried[0], again, (~fits, result))[1]


def on_device(resident, factor, dinv, panel_cols, row_lists):
    matrix = resident
    for panel in reversed(range(factor.shape[0])):
        matrix = panel_step(
            matrix, factor[panel], dinv[panel], panel_cols[panel], row_lists[panel]
        )
    return matrix


def solution(mesh):
    finer = Mesh(
        mesh.devices.reshape(-1, 2, 2, mesh.shape["col"]), ("row_0", "row_1", "row_2", "col")
    )
    return jax.shard_map(
        on_device,
        mesh=finer,
        in_specs=(P(ROW, "col"), P(None, "col", ROW), P(None, "col", None), P(), P()),
        out_specs=P(ROW, "col"),
        check_vma=False,
    )
```

```python
import functools

import jax
import jax.numpy as jnp
from jax import lax
from jax.experimental import pallas as pl
from jax.experimental.pallas import tpu as pltpu
from jax.sharding import Mesh
from jax.sharding import PartitionSpec as P

ROW = ("row_0", "row_1", "row_2")
HIGHEST = lax.Precision.HIGHEST
LANES = 128
LINES = 16
BY_LAST = ((1,), (1,))
BY_FIRST = ((0,), (0,))


def dot(a, b, dims=((1,), (0,))):
    return lax.dot_general(
        a, b, (dims, ((), ())), precision=HIGHEST, preferred_element_type=jnp.float32
    )


def thirds(values, axis):
    high = lax.reduce_precision(values, 8, 7)
    rest = values - high
    middle = lax.reduce_precision(rest, 8, 7)
    parts = [part.astype(jnp.bfloat16) for part in (high, middle, rest - middle)]
    return jnp.concatenate(parts, axis=axis)


def selected(parts, hot, dims=((1,), (0,))):
    out = lax.dot_general(
        parts, hot, (dims, ((), ())), preferred_element_type=jnp.float32
    )
    size = out.shape[0] // 3
    return out[:size] + out[size : 2 * size] + out[2 * size :]


def sum_at_owner(blocks, axis):
    return jnp.sum(lax.all_to_all(blocks, axis, 0, 0, tiled=True), axis=0)


def sent_to_all(shard, axis):
    copies = jnp.broadcast_to(shard, (lax.axis_size(axis), *shard.shape))
    return lax.all_to_all(copies, axis, split_axis=0, concat_axis=0, tiled=True)


def ring_sum(shard, axis):
    count = lax.axis_size(axis)
    ring = [(place, (place + 1) % count) for place in range(count)]

    def step(_, carried):
        moving, total = carried
        moving = lax.ppermute(moving, axis, ring)
        return moving, total + moving

    return lax.fori_loop(0, count - 1, step, (shard, shard))[1]


def general_panel(matrix, factor, dinv, panel_cols, row_in, col_in):
    row_count = lax.axis_size(ROW)
    ratio = lax.axis_size("col") // row_count
    row_block, col_block = matrix.shape
    width = panel_cols.shape[0]
    group = factor.shape[1]
    row_pos = lax.axis_index(ROW)
    col_pos = lax.axis_index("col")
    row_ids = row_pos * row_block + jnp.arange(row_block, dtype=jnp.int32)
    col_ids = col_pos * col_block + jnp.arange(col_block, dtype=jnp.int32)
    masked = factor * col_in[:, None].astype(jnp.float32)

    def column_places(turn):
        cols = lax.dynamic_slice_in_dim(panel_cols, turn * group, group)
        return cols, (cols[:, None] == col_ids).astype(jnp.float32)

    def products(turn, carried):
        out, gram = carried
        lower = ring_sum(jnp.where(row_pos == turn, masked, jnp.zeros_like(masked)), ROW)
        by_row = ring_sum(-dot(matrix, lower), "col")
        mine = lax.dynamic_slice_in_dim(by_row, col_pos % ratio * col_block, col_block, 0)
        mine = jnp.where(row_pos == col_pos // ratio, mine, jnp.zeros_like(mine))
        by_col = ring_sum(mine, ROW)
        gram = lax.dynamic_update_slice(
            gram, dot(masked, by_col, BY_FIRST), (row_pos * group, turn * group)
        )
        cols, put_cols = column_places(turn)
        put_rows = (row_ids[:, None] == cols).astype(jnp.float32)
        here = jnp.sum(put_cols, axis=0) > 0.5
        there = jnp.sum(put_rows, axis=1) > 0.5
        out = jnp.where(
            row_in[:, None] & here[None, :],
            dot(by_row, put_cols),
            jnp.where(there[:, None] & col_in[None, :], dot(put_rows, by_col, BY_LAST), out),
        )
        return out, gram

    none = jnp.zeros((width, width), jnp.float32)
    out, gram = lax.fori_loop(0, row_count, products, (matrix, none))
    placed = lax.dynamic_update_slice(none, dinv, (col_pos * dinv.shape[0], 0))
    placed = jnp.where(row_pos == 0, placed, none)
    diagonal = ring_sum(ring_sum(placed - gram, ROW), "col")
    put_rows = (row_ids[:, None] == panel_cols).astype(jnp.float32)
    there = jnp.sum(put_rows, axis=1) > 0.5

    def corners(turn, out):
        _, put_cols = column_places(turn)
        here = jnp.sum(put_cols, axis=0) > 0.5
        part = lax.dynamic_slice_in_dim(diagonal, turn * group, group, 1)
        corner = dot(dot(put_rows, part), put_cols)
        return jnp.where(there[:, None] & here[None, :], corner, out)

    return lax.fori_loop(0, row_count, corners, out)


def slots_kernel(lines, lanes, device_ref, rows_ref, cols_ref, row_slots_ref, col_slots_ref):
    line = lax.broadcasted_iota(jnp.int32, (LINES, 1), 0)
    own = jnp.where(
        line < lines, device_ref[0] * lines + line, device_ref[1] * lines + line - lines
    )
    lower = lax.broadcasted_iota(jnp.int32, (lanes, lanes), 0)
    upper = lax.broadcasted_iota(jnp.int32, (lanes, lanes), 1)
    earlier = (lower < upper).astype(jnp.float32)
    for listed_ref, out_ref in ((rows_ref, row_slots_ref), (cols_ref, col_slots_ref)):
        count = listed_ref.shape[1]
        step = min(count, 1024)
        found = jnp.zeros((LINES, lanes), jnp.float32)
        for start in range(0, count, step):
            size = min(step, count - start)
            listed = listed_ref[:, start : start + size]
            high = lax.div(listed, jnp.int32(lanes))
            low = listed - high * lanes
            line_hit = (own == high).astype(jnp.float32)
            lane_hit = lax.broadcasted_iota(jnp.int32, (lanes, size), 0) == low
            found += lax.dot_general(
                line_hit.astype(jnp.bfloat16),
                lane_hit.astype(jnp.float32).astype(jnp.bfloat16),
                (BY_LAST, ((), ())),
                preferred_element_type=jnp.float32,
            )
        before = jnp.dot(
            found.astype(jnp.bfloat16),
            earlier.astype(jnp.bfloat16),
            preferred_element_type=jnp.float32,
        )
        held = jnp.sum(found, axis=1, keepdims=True)
        for other in range(LINES):
            if (other + 1) % lines:
                later = (line > other) & (line < (other // lines + 1) * lines)
                before += jnp.where(later, held[other : other + 1], 0.0)
        out_ref[...] = jnp.where(found > 0.5, before, -1.0).astype(jnp.int32)


def block_slots(col_block, ratio, panel_cols, row_lists):
    lanes = LANES if col_block % LANES == 0 else col_block
    lines = col_block // lanes
    device = jnp.stack([lax.axis_index("col"), lax.axis_index(ROW) * ratio]).astype(jnp.int32)
    shape = jax.ShapeDtypeStruct((LINES, lanes), jnp.int32)
    whole = pl.BlockSpec(memory_space=pltpu.VMEM)
    found = pl.pallas_call(
        functools.partial(slots_kernel, lines, lanes),
        out_shape=(shape, shape),
        in_specs=[pl.BlockSpec(memory_space=pltpu.SMEM), whole, whole],
        out_specs=(whole, whole),
        name="block_slots",
    )(device, row_lists[None], panel_cols[None])
    used = (1 + ratio) * lines
    return [slots[:used].reshape(used * lanes) for slots in found]


def one_hot(slot, count, dtype=jnp.float32):
    hot = slot[:, None] == jnp.arange(count, dtype=jnp.int32)
    return hot.astype(jnp.float32).astype(dtype)


def fullest(listed, col_block, col_count):
    home = listed // col_block
    counts = jnp.sum((jnp.arange(col_count)[:, None] == home).astype(jnp.int32), axis=1)
    return jnp.max(counts)


def panel_step(matrix, factor, dinv, panel_cols, row_lists):
    row_count = lax.axis_size(ROW)
    col_count = lax.axis_size("col")
    ratio = col_count // row_count
    row_block, col_block = matrix.shape
    width = panel_cols.shape[0]
    dinv_rows = dinv.shape[0]
    row_slots = col_block * 2 // 3
    col_slots = 2 * (width // col_count)
    row_k = ratio * col_slots
    row_pos = lax.axis_index(ROW)
    col_pos = lax.axis_index("col")
    side = col_pos % ratio

    list_slot, panel_slot = block_slots(col_block, ratio, panel_cols, row_lists)
    in_list, in_panel = list_slot >= 0, panel_slot >= 0
    col_in, row_in = in_list[:col_block], in_list[col_block:]
    col_panel, row_panel = in_panel[:col_block], in_panel[col_block:]
    pick = one_hot(list_slot, row_slots)
    pick_cols = pick[:col_block]
    pick_rows = pick[col_block:].reshape(ratio, col_block, row_slots)
    put = one_hot(panel_slot, col_slots)
    put_cols = put[:col_block]
    put_rows = put[col_block:].reshape(ratio, col_block, col_slots)

    narrow_pick = one_hot(list_slot[:col_block], row_slots, jnp.bfloat16)
    packed = selected(thirds(factor, 1), narrow_pick, BY_FIRST)
    own_half = sent_to_all(packed, ROW[:2]).reshape(width // 2, row_slots)
    other_half = lax.ppermute(own_half, ROW[2], [(0, 1), (1, 0)])
    lower = jnp.concatenate([own_half, other_half])

    narrow = dot(matrix, pick_cols).reshape(ratio, col_block, row_slots)
    dense = jnp.stack([dot(pick_rows[part], narrow[part], BY_FIRST) for part in range(ratio)])
    share = row_slots // col_count
    dense = jnp.moveaxis(dense.reshape(ratio, col_count, share, row_slots), 0, 1)
    dense = dense.reshape(ratio * row_slots, row_slots)

    partial_value = -dot(dense, lower, BY_LAST)
    summed = sum_at_owner(partial_value.reshape(col_count, ratio * share, width), "col")

    home = panel_cols // col_block
    earlier = (panel_cols[None, :] < panel_cols[:, None]) & (home[None, :] == home[:, None])
    rank = jnp.sum(earlier.astype(jnp.int32), axis=1)
    slot = home * col_slots + rank
    wide = ratio * row_k
    pair = home // ratio * wide
    place = home % ratio
    half_slots = col_slots // 2

    def this_core_first(values):
        by_core = jnp.moveaxis(values.reshape(-1, 2, factor.shape[1]), 1, 0)
        by_core = by_core.reshape(2, width // 2)
        return jnp.where(lax.axis_index(ROW[2]) == 0, by_core, by_core[::-1]).reshape(width)

    def route(first):
        places = [this_core_first(first(part)) for part in range(ratio)]
        return one_hot(jnp.concatenate(places), row_count * wide, jnp.bfloat16)

    to_rows = route(lambda part: pair + part * row_k + place * col_slots + rank)
    to_cols = route(lambda part: pair + (1 - place) * row_k + part * col_slots + rank)

    halves_beside = jnp.concatenate([summed[:share], summed[share:]], axis=1)
    parts = thirds(halves_beside, 0)
    chosen = selected(parts, to_rows).reshape(share, row_count, wide)
    received = lax.all_to_all(jnp.moveaxis(chosen, 1, 0), ROW, 0, 0, tiled=True)

    own = jnp.moveaxis(selected(parts, to_cols).reshape(share, row_count, wide), 1, 0)
    lane = jnp.arange(wide, dtype=jnp.int32) // row_k
    sent = jnp.stack([jnp.where(lane == part, received, own) for part in range(ratio)], axis=1)
    arrived = lax.all_to_all(
        sent.reshape(col_count, share, wide), "col", 0, 0, tiled=True
    )
    arrived = arrived.reshape(row_slots, wide).T
    upper, under = arrived[:row_k], arrived[row_k:]
    beside = jnp.where(side == 0, upper, under)
    below = jnp.where(side == 0, under, upper)

    def halves(values):
        blocks = values.reshape(col_count, 2, half_slots, values.shape[1])
        return [blocks[:, part].reshape(col_count * half_slots, -1) for part in range(2)]

    slots = col_count * col_slots
    lower_slots = dot(one_hot(this_core_first(slot), slots), lower, BY_FIRST)
    mine = lax.dynamic_slice_in_dim(slot, col_pos * dinv_rows, dinv_rows)
    placed = dot(
        one_hot(mine, slots), dot(dinv, one_hot(slot - row_pos * row_k, row_k)), BY_FIRST
    )
    lower_pair = jnp.concatenate(halves(lower_slots), axis=1)
    placed_pair = jnp.concatenate(halves(placed), axis=1)
    empty = jnp.zeros_like(beside)
    beside_pair = jnp.concatenate(
        [jnp.concatenate([beside, empty], axis=1), jnp.concatenate([empty, beside], axis=1)]
    )
    terms = placed_pair - dot(lower_pair, beside_pair, BY_LAST)
    corner = sum_at_owner(terms.reshape(col_count, half_slots, 2 * row_k), "col")

    below_rows = [dot(pick_rows[part], below[part * col_slots : (part + 1) * col_slots], BY_LAST) for part in range(ratio)]
    spread_out = dot(beside, pick_cols, BY_LAST)
    at_rows = jnp.concatenate(
        [
            dot(put_rows[part], spread_out[part * col_slots : (part + 1) * col_slots])
            for part in range(ratio)
        ]
    )
    with_rows = jnp.where(row_panel[:, None] & col_in[None, :], at_rows, matrix)
    at_cols = jnp.concatenate(
        [
            below_rows[part]
            + jnp.concatenate(
                [
                    dot(
                        put_rows[part],
                        corner[:, (half * ratio + part) * col_slots :][:, :col_slots],
                        BY_LAST,
                    )
                    for half in range(2)
                ],
                axis=1,
            )
            for part in range(ratio)
        ]
    )
    taken_over = (row_panel | row_in)[:, None] & col_panel[None, :]
    result = jnp.where(taken_over, dot(at_cols, put_cols, BY_LAST), with_rows)

    fits = (fullest(row_lists, col_block, col_count) <= row_slots) & (
        fullest(panel_cols, col_block, col_count) <= col_slots
    )

    def again(carried):
        general = general_panel(matrix, factor, dinv, panel_cols, row_in, col_in)
        return jnp.zeros((), jnp.bool_), general

    return lax.while_loop(lambda carried: carried[0], again, (~fits, result))[1]


def on_device(resident, factor, dinv, panel_cols, row_lists):
    matrix = resident
    for panel in reversed(range(factor.shape[0])):
        matrix = panel_step(
            matrix, factor[panel], dinv[panel], panel_cols[panel], row_lists[panel]
        )
    return matrix


def solution(mesh):
    finer = Mesh(
        mesh.devices.reshape(-1, 2, 2, mesh.shape["col"]), ("row_0", "row_1", "row_2", "col")
    )
    return jax.shard_map(
        on_device,
        mesh=finer,
        in_specs=(P(ROW, "col"), P(None, "col", ROW), P(None, "col", None), P(), P()),
        out_specs=P(ROW, "col"),
        check_vma=False,
    )
```

```python
import functools

import jax
import jax.numpy as jnp
from jax import lax
from jax.experimental import pallas as pl
from jax.experimental.pallas import tpu as pltpu
from jax.sharding import Mesh
from jax.sharding import PartitionSpec as P

ROW = ("row_0", "row_1", "row_2")
HIGHEST = lax.Precision.HIGHEST
LANES = 128
LINES = 16
BY_LAST = ((1,), (1,))
BY_FIRST = ((0,), (0,))


def dot(a, b, dims=((1,), (0,))):
    return lax.dot_general(
        a, b, (dims, ((), ())), precision=HIGHEST, preferred_element_type=jnp.float32
    )


def thirds(values, axis):
    high = lax.reduce_precision(values, 8, 7)
    rest = values - high
    middle = lax.reduce_precision(rest, 8, 7)
    parts = [part.astype(jnp.bfloat16) for part in (high, middle, rest - middle)]
    return jnp.concatenate(parts, axis=axis)


def selected(parts, hot, dims=((1,), (0,))):
    out = lax.dot_general(
        parts, hot, (dims, ((), ())), preferred_element_type=jnp.float32
    )
    size = out.shape[0] // 3
    return out[:size] + out[size : 2 * size] + out[2 * size :]


def sum_at_owner(blocks, axis):
    return jnp.sum(lax.all_to_all(blocks, axis, 0, 0, tiled=True), axis=0)


def ring_sum(shard, axis):
    count = lax.axis_size(axis)
    ring = [(place, (place + 1) % count) for place in range(count)]

    def step(_, carried):
        moving, total = carried
        moving = lax.ppermute(moving, axis, ring)
        return moving, total + moving

    return lax.fori_loop(0, count - 1, step, (shard, shard))[1]


def general_panel(matrix, factor, dinv, panel_cols, row_in, col_in):
    row_count = lax.axis_size(ROW)
    ratio = lax.axis_size("col") // row_count
    row_block, col_block = matrix.shape
    width = panel_cols.shape[0]
    group = factor.shape[1]
    row_pos = lax.axis_index(ROW)
    col_pos = lax.axis_index("col")
    row_ids = row_pos * row_block + jnp.arange(row_block, dtype=jnp.int32)
    col_ids = col_pos * col_block + jnp.arange(col_block, dtype=jnp.int32)
    masked = factor * col_in[:, None].astype(jnp.float32)

    def column_places(turn):
        cols = lax.dynamic_slice_in_dim(panel_cols, turn * group, group)
        return cols, (cols[:, None] == col_ids).astype(jnp.float32)

    def products(turn, carried):
        out, gram = carried
        lower = ring_sum(jnp.where(row_pos == turn, masked, jnp.zeros_like(masked)), ROW)
        by_row = ring_sum(-dot(matrix, lower), "col")
        mine = lax.dynamic_slice_in_dim(by_row, col_pos % ratio * col_block, col_block, 0)
        mine = jnp.where(row_pos == col_pos // ratio, mine, jnp.zeros_like(mine))
        by_col = ring_sum(mine, ROW)
        gram = lax.dynamic_update_slice(
            gram, dot(masked, by_col, BY_FIRST), (row_pos * group, turn * group)
        )
        cols, put_cols = column_places(turn)
        put_rows = (row_ids[:, None] == cols).astype(jnp.float32)
        here = jnp.sum(put_cols, axis=0) > 0.5
        there = jnp.sum(put_rows, axis=1) > 0.5
        out = jnp.where(
            row_in[:, None] & here[None, :],
            dot(by_row, put_cols),
            jnp.where(there[:, None] & col_in[None, :], dot(put_rows, by_col, BY_LAST), out),
        )
        return out, gram

    none = jnp.zeros((width, width), jnp.float32)
    out, gram = lax.fori_loop(0, row_count, products, (matrix, none))
    placed = lax.dynamic_update_slice(none, dinv, (col_pos * dinv.shape[0], 0))
    placed = jnp.where(row_pos == 0, placed, none)
    diagonal = ring_sum(ring_sum(placed - gram, ROW), "col")
    put_rows = (row_ids[:, None] == panel_cols).astype(jnp.float32)
    there = jnp.sum(put_rows, axis=1) > 0.5

    def corners(turn, out):
        _, put_cols = column_places(turn)
        here = jnp.sum(put_cols, axis=0) > 0.5
        part = lax.dynamic_slice_in_dim(diagonal, turn * group, group, 1)
        corner = dot(dot(put_rows, part), put_cols)
        return jnp.where(there[:, None] & here[None, :], corner, out)

    return lax.fori_loop(0, row_count, corners, out)


def slots_kernel(
    lines, lanes, device_ref, rows_ref, cols_ref, factor_ref, row_slots_ref, col_slots_ref, packed_ref
):
    line = lax.broadcasted_iota(jnp.int32, (LINES, 1), 0)
    own = jnp.where(
        line < lines, device_ref[0] * lines + line, device_ref[1] * lines + line - lines
    )
    lower = lax.broadcasted_iota(jnp.int32, (lanes, lanes), 0)
    upper = lax.broadcasted_iota(jnp.int32, (lanes, lanes), 1)
    earlier = (lower < upper).astype(jnp.float32)
    for listed_ref, out_ref in ((rows_ref, row_slots_ref), (cols_ref, col_slots_ref)):
        count = listed_ref.shape[1]
        step = min(count, 1024)
        found = jnp.zeros((LINES, lanes), jnp.float32)
        for start in range(0, count, step):
            size = min(step, count - start)
            listed = listed_ref[:, start : start + size]
            high = lax.div(listed, jnp.int32(lanes))
            low = listed - high * lanes
            line_hit = (own == high).astype(jnp.float32)
            lane_hit = lax.broadcasted_iota(jnp.int32, (lanes, size), 0) == low
            found += lax.dot_general(
                line_hit.astype(jnp.bfloat16),
                lane_hit.astype(jnp.float32).astype(jnp.bfloat16),
                (BY_LAST, ((), ())),
                preferred_element_type=jnp.float32,
            )
        before = jnp.dot(
            found.astype(jnp.bfloat16),
            earlier.astype(jnp.bfloat16),
            preferred_element_type=jnp.float32,
        )
        held = jnp.sum(found, axis=1, keepdims=True)
        for other in range(LINES):
            if (other + 1) % lines:
                later = (line > other) & (line < (other // lines + 1) * lines)
                before += jnp.where(later, held[other : other + 1], 0.0)
        out_ref[...] = jnp.where(found > 0.5, before, -1.0).astype(jnp.int32)
    copies, group, slots = packed_ref.shape
    place = lax.broadcasted_iota(jnp.int32, (slots, lanes), 0)
    packed = jnp.zeros((slots, group), jnp.float32)
    for part in range(lines):
        hot = (place == row_slots_ref[part : part + 1, :]).astype(jnp.float32)
        held = factor_ref[part * lanes : (part + 1) * lanes, :]
        packed += jnp.dot(hot, held, precision=HIGHEST, preferred_element_type=jnp.float32)
    packed_ref[...] = jnp.broadcast_to(packed.T[None], packed_ref.shape)


def block_slots(row_slots, ratio, factor, panel_cols, row_lists):
    col_block, group = factor.shape
    copies = lax.axis_size(ROW[:2])
    lanes = LANES if col_block % LANES == 0 else col_block
    lines = col_block // lanes
    device = jnp.stack([lax.axis_index("col"), lax.axis_index(ROW) * ratio]).astype(jnp.int32)
    shape = jax.ShapeDtypeStruct((LINES, lanes), jnp.int32)
    whole = pl.BlockSpec(memory_space=pltpu.VMEM)
    found = pl.pallas_call(
        functools.partial(slots_kernel, lines, lanes),
        out_shape=(shape, shape, jax.ShapeDtypeStruct((copies, group, row_slots), jnp.float32)),
        in_specs=[pl.BlockSpec(memory_space=pltpu.SMEM), whole, whole, whole],
        out_specs=(whole, whole, whole),
        name="block_slots",
    )(device, row_lists[None], panel_cols[None], factor)
    used = (1 + ratio) * lines
    return [slots[:used].reshape(used * lanes) for slots in found[:2]] + [found[2]]


def one_hot(slot, count, dtype=jnp.float32):
    hot = slot[:, None] == jnp.arange(count, dtype=jnp.int32)
    return hot.astype(jnp.float32).astype(dtype)


def places_kernel(sizes, panel_ref, other_ref, rows_ref, out_ref):
    col_block, ratio, col_slots, col_count = sizes
    row_k = ratio * col_slots
    wide = ratio * row_k
    other = other_ref[...]
    other_home = lax.div(other, jnp.int32(col_block))
    for order in range(2):
        panel = panel_ref[order : order + 1, :]
        home = lax.div(panel, jnp.int32(col_block))
        earlier = (other < panel) & (other_home == home)
        rank = jnp.sum(earlier.astype(jnp.float32), axis=0, keepdims=True).astype(jnp.int32)
        pair = lax.div(home, jnp.int32(ratio))
        place = home - pair * ratio
        out_ref[order : order + 1, :] = home * col_slots + rank
    for part in range(ratio):
        down = pair * wide + part * row_k + place * col_slots + rank
        along = pair * wide + (1 - place) * row_k + part * col_slots + rank
        out_ref[2 + part : 3 + part, :] = down
        out_ref[2 + ratio + part : 3 + ratio + part, :] = along
    out_ref[6:7, :] = rank
    rows_home = lax.div(rows_ref[...], jnp.int32(col_block))
    block = lax.broadcasted_iota(jnp.int32, (col_count, rows_ref.shape[1]), 0)
    counts = jnp.sum((block == rows_home).astype(jnp.float32), axis=1, keepdims=True)
    most = jnp.max(counts, axis=0, keepdims=True).astype(jnp.int32)
    out_ref[7:8, :] = jnp.broadcast_to(most, (1, panel_ref.shape[1]))


def panel_places(col_slots, col_block, ratio, col_count, group, panel_cols, row_lists):
    width = panel_cols.shape[0]
    by_core = jnp.moveaxis(panel_cols.reshape(-1, 2, group), 1, 0).reshape(2, width // 2)
    local = jnp.where(lax.axis_index(ROW[2]) == 0, by_core, by_core[::-1]).reshape(width)
    return pl.pallas_call(
        functools.partial(places_kernel, (col_block, ratio, col_slots, col_count)),
        out_shape=jax.ShapeDtypeStruct((8, width), jnp.int32),
        name="panel_places",
    )(jnp.stack([panel_cols, local]), panel_cols[:, None], row_lists[None])


def panel_step(matrix, factor, dinv, panel_cols, row_lists):
    row_count = lax.axis_size(ROW)
    col_count = lax.axis_size("col")
    ratio = col_count // row_count
    row_block, col_block = matrix.shape
    width = panel_cols.shape[0]
    dinv_rows = dinv.shape[0]
    row_slots = col_block * 2 // 3
    col_slots = 2 * (width // col_count)
    row_k = ratio * col_slots
    row_pos = lax.axis_index(ROW)
    col_pos = lax.axis_index("col")
    side = col_pos % ratio

    list_slot, panel_slot, packed = block_slots(
        row_slots, ratio, factor, panel_cols, row_lists
    )
    in_list, in_panel = list_slot >= 0, panel_slot >= 0
    col_in, row_in = in_list[:col_block], in_list[col_block:]
    col_panel, row_panel = in_panel[:col_block], in_panel[col_block:]
    pick = one_hot(list_slot, row_slots)
    pick_cols = pick[:col_block]
    pick_rows = pick[col_block:].reshape(ratio, col_block, row_slots)
    put = one_hot(panel_slot, col_slots)
    put_rows = put[col_block:].reshape(ratio, col_block, col_slots)

    own_half = lax.all_to_all(packed, ROW[:2], 0, 0, tiled=True)
    own_half = own_half.reshape(width // 2, row_slots)
    other_half = lax.ppermute(own_half, ROW[2], [(0, 1), (1, 0)])
    lower = jnp.concatenate([own_half, other_half])

    narrow = dot(matrix, pick_cols).reshape(ratio, col_block, row_slots)
    dense = jnp.stack([dot(pick_rows[part], narrow[part], BY_FIRST) for part in range(ratio)])
    share = row_slots // col_count
    dense = jnp.moveaxis(dense.reshape(ratio, col_count, share, row_slots), 0, 1)
    dense = dense.reshape(ratio * row_slots, row_slots)

    partial_value = -dot(dense, lower, BY_LAST)
    summed = sum_at_owner(partial_value.reshape(col_count, ratio * share, width), "col")

    wide = ratio * row_k
    half_slots = col_slots // 2
    slots = col_count * col_slots
    found = panel_places(
        col_slots, col_block, ratio, col_count, factor.shape[1], panel_cols, row_lists
    )
    slot, local_slot = found[0], found[1]

    def route(places):
        return one_hot(places.reshape(ratio * width), row_count * wide, jnp.bfloat16)

    to_rows = route(found[2:4])
    to_cols = route(found[4:6])

    halves_beside = jnp.concatenate([summed[:share], summed[share:]], axis=1)
    parts = thirds(halves_beside, 0)
    chosen = selected(parts, to_rows).reshape(share, row_count, wide)
    received = lax.all_to_all(jnp.moveaxis(chosen, 1, 0), ROW, 0, 0, tiled=True)

    own = jnp.moveaxis(selected(parts, to_cols).reshape(share, row_count, wide), 1, 0)
    lane = jnp.arange(wide, dtype=jnp.int32) // row_k
    sent = jnp.stack([jnp.where(lane == part, received, own) for part in range(ratio)], axis=1)
    arrived = lax.all_to_all(
        sent.reshape(col_count, share, wide), "col", 0, 0, tiled=True
    )
    arrived = arrived.reshape(row_slots, wide).T
    upper, under = arrived[:row_k], arrived[row_k:]
    beside = jnp.where(side == 0, upper, under)
    below = jnp.where(side == 0, under, upper)

    def halves(values):
        blocks = values.reshape(col_count, 2, half_slots, values.shape[1])
        return [blocks[:, part].reshape(col_count * half_slots, -1) for part in range(2)]

    lower_slots = dot(one_hot(local_slot, slots), lower, BY_FIRST)
    mine = lax.dynamic_slice_in_dim(slot, col_pos * dinv_rows, dinv_rows)
    placed = dot(
        one_hot(mine, slots), dot(dinv, one_hot(slot - row_pos * row_k, row_k)), BY_FIRST
    )
    lower_pair = jnp.concatenate(halves(lower_slots), axis=1)
    placed_pair = jnp.concatenate(halves(placed), axis=1)
    empty = jnp.zeros_like(beside)
    beside_pair = jnp.concatenate(
        [jnp.concatenate([beside, empty], axis=1), jnp.concatenate([empty, beside], axis=1)]
    )
    terms = placed_pair - dot(lower_pair, beside_pair, BY_LAST)
    corner = sum_at_owner(terms.reshape(col_count, half_slots, 2 * row_k), "col")

    below_rows = [dot(pick_rows[part], below[part * col_slots : (part + 1) * col_slots], BY_LAST) for part in range(ratio)]
    spread_out = dot(beside, pick_cols, BY_LAST)
    at_rows = jnp.concatenate(
        [
            dot(put_rows[part], spread_out[part * col_slots : (part + 1) * col_slots])
            for part in range(ratio)
        ]
    )
    with_rows = jnp.where(row_panel[:, None] & col_in[None, :], at_rows, matrix)
    corner = jnp.concatenate([corner[:, :row_k], corner[:, row_k:]])
    at_cols = jnp.concatenate(
        [
            below_rows[part]
            + dot(
                put_rows[part],
                corner[:, part * col_slots : (part + 1) * col_slots],
                BY_LAST,
            )
            for part in range(ratio)
        ]
    )
    thrice = jnp.concatenate([one_hot(panel_slot[:col_block], col_slots, jnp.bfloat16)] * 3, axis=1)
    at_cols = lax.dot_general(
        thirds(at_cols, 1),
        thrice,
        (BY_LAST, ((), ())),
        preferred_element_type=jnp.float32,
    )
    taken_over = (row_panel | row_in)[:, None] & col_panel[None, :]
    result = jnp.where(taken_over, at_cols, with_rows)

    fits = (jnp.max(found[6]) < col_slots) & (jnp.max(found[7]) <= row_slots)

    def again(carried):
        general = general_panel(matrix, factor, dinv, panel_cols, row_in, col_in)
        return jnp.zeros((), jnp.bool_), general

    return lax.while_loop(lambda carried: carried[0], again, (~fits, result))[1]


def on_device(resident, factor, dinv, panel_cols, row_lists):
    matrix = resident
    for panel in reversed(range(factor.shape[0])):
        matrix = panel_step(
            matrix, factor[panel], dinv[panel], panel_cols[panel], row_lists[panel]
        )
    return matrix


def solution(mesh):
    finer = Mesh(
        mesh.devices.reshape(-1, 2, 2, mesh.shape["col"]), ("row_0", "row_1", "row_2", "col")
    )
    return jax.shard_map(
        on_device,
        mesh=finer,
        in_specs=(P(ROW, "col"), P(None, "col", ROW), P(None, "col", None), P(), P()),
        out_specs=P(ROW, "col"),
        check_vma=False,
    )
```

```python
import functools

import jax
import jax.numpy as jnp
from jax import lax
from jax.experimental import pallas as pl
from jax.experimental.pallas import tpu as pltpu
from jax.sharding import Mesh
from jax.sharding import PartitionSpec as P


ROW = ("row_0", "row_1", "row_2")
COL = ("col_0", "col_1")
HIGHEST = lax.Precision.HIGHEST
LANES = 128
LINES = 16
BY_LAST = ((1,), (1,))
BY_FIRST = ((0,), (0,))


def dot(a, b, dims=((1,), (0,))):
    return lax.dot_general(
        a, b, (dims, ((), ())), precision=HIGHEST, preferred_element_type=jnp.float32
    )


def thirds(values, axis):
    high = lax.reduce_precision(values, 8, 7)
    rest = values - high
    middle = lax.reduce_precision(rest, 8, 7)
    parts = [part.astype(jnp.bfloat16) for part in (high, middle, rest - middle)]
    return jnp.concatenate(parts, axis=axis)


def selected(parts, hot, dims=((1,), (0,))):
    out = lax.dot_general(
        parts, hot, (dims, ((), ())), preferred_element_type=jnp.float32
    )
    size = out.shape[0] // 3
    return out[:size] + out[size : 2 * size] + out[2 * size :]


def sum_at_owner(blocks, axis):
    return jnp.sum(lax.all_to_all(blocks, axis, 0, 0, tiled=True), axis=0)


def ring_sum(shard, axis):
    count = lax.axis_size(axis)
    ring = [(place, (place + 1) % count) for place in range(count)]

    def step(_, carried):
        moving, total = carried
        moving = lax.ppermute(moving, axis, ring)
        return moving, total + moving

    return lax.fori_loop(0, count - 1, step, (shard, shard))[1]


def general_panel(matrix, factor, dinv, panel_cols, row_in, col_in):
    row_count = lax.axis_size(ROW)
    ratio = lax.axis_size(COL) // row_count
    row_block, col_block = matrix.shape
    width = panel_cols.shape[0]
    group = factor.shape[1]
    row_pos = lax.axis_index(ROW)
    col_pos = lax.axis_index(COL)
    row_ids = row_pos * row_block + jnp.arange(row_block, dtype=jnp.int32)
    col_ids = col_pos * col_block + jnp.arange(col_block, dtype=jnp.int32)
    masked = factor * col_in[:, None].astype(jnp.float32)

    def column_places(turn):
        cols = lax.dynamic_slice_in_dim(panel_cols, turn * group, group)
        return cols, (cols[:, None] == col_ids).astype(jnp.float32)

    def products(turn, carried):
        out, gram = carried
        lower = ring_sum(jnp.where(row_pos == turn, masked, jnp.zeros_like(masked)), ROW)
        by_row = ring_sum(-dot(matrix, lower), COL)
        mine = lax.dynamic_slice_in_dim(by_row, col_pos % ratio * col_block, col_block, 0)
        mine = jnp.where(row_pos == col_pos // ratio, mine, jnp.zeros_like(mine))
        by_col = ring_sum(mine, ROW)
        gram = lax.dynamic_update_slice(
            gram, dot(masked, by_col, BY_FIRST), (row_pos * group, turn * group)
        )
        cols, put_cols = column_places(turn)
        put_rows = (row_ids[:, None] == cols).astype(jnp.float32)
        here = jnp.sum(put_cols, axis=0) > 0.5
        there = jnp.sum(put_rows, axis=1) > 0.5
        out = jnp.where(
            row_in[:, None] & here[None, :],
            dot(by_row, put_cols),
            jnp.where(there[:, None] & col_in[None, :], dot(put_rows, by_col, BY_LAST), out),
        )
        return out, gram

    none = jnp.zeros((width, width), jnp.float32)
    out, gram = lax.fori_loop(0, row_count, products, (matrix, none))
    placed = lax.dynamic_update_slice(none, dinv, (col_pos * dinv.shape[0], 0))
    placed = jnp.where(row_pos == 0, placed, none)
    diagonal = ring_sum(ring_sum(placed - gram, ROW), COL)
    put_rows = (row_ids[:, None] == panel_cols).astype(jnp.float32)
    there = jnp.sum(put_rows, axis=1) > 0.5

    def corners(turn, out):
        _, put_cols = column_places(turn)
        here = jnp.sum(put_cols, axis=0) > 0.5
        part = lax.dynamic_slice_in_dim(diagonal, turn * group, group, 1)
        corner = dot(dot(put_rows, part), put_cols)
        return jnp.where(there[:, None] & here[None, :], corner, out)

    return lax.fori_loop(0, row_count, corners, out)


def slots_kernel(lines, lanes, device_ref, rows_ref, cols_ref, row_slots_ref, col_slots_ref):
    line = lax.broadcasted_iota(jnp.int32, (LINES, 1), 0)
    own = jnp.where(
        line < lines, device_ref[0] * lines + line, device_ref[1] * lines + line - lines
    )
    lower = lax.broadcasted_iota(jnp.int32, (lanes, lanes), 0)
    upper = lax.broadcasted_iota(jnp.int32, (lanes, lanes), 1)
    earlier = (lower < upper).astype(jnp.float32)
    for listed_ref, out_ref in ((rows_ref, row_slots_ref), (cols_ref, col_slots_ref)):
        count = listed_ref.shape[1]
        step = min(count, 1024)
        found = jnp.zeros((LINES, lanes), jnp.float32)
        for start in range(0, count, step):
            size = min(step, count - start)
            listed = listed_ref[:, start : start + size]
            high = lax.div(listed, jnp.int32(lanes))
            low = listed - high * lanes
            line_hit = (own == high).astype(jnp.float32)
            lane_hit = lax.broadcasted_iota(jnp.int32, (lanes, size), 0) == low
            found += lax.dot_general(
                line_hit.astype(jnp.bfloat16),
                lane_hit.astype(jnp.float32).astype(jnp.bfloat16),
                (BY_LAST, ((), ())),
                preferred_element_type=jnp.float32,
            )
        before = jnp.dot(
            found.astype(jnp.bfloat16),
            earlier.astype(jnp.bfloat16),
            preferred_element_type=jnp.float32,
        )
        held = jnp.sum(found, axis=1, keepdims=True)
        for other in range(LINES):
            if (other + 1) % lines:
                later = (line > other) & (line < (other // lines + 1) * lines)
                before += jnp.where(later, held[other : other + 1], 0.0)
        out_ref[...] = jnp.where(found > 0.5, before, -1.0).astype(jnp.int32)


def block_slots(col_block, ratio, panel_cols, row_lists):
    lanes = LANES if col_block % LANES == 0 else col_block
    lines = col_block // lanes
    device = jnp.stack([lax.axis_index(COL), lax.axis_index(ROW) * ratio]).astype(jnp.int32)
    shape = jax.ShapeDtypeStruct((LINES, lanes), jnp.int32)
    whole = pl.BlockSpec(memory_space=pltpu.VMEM)
    found = pl.pallas_call(
        functools.partial(slots_kernel, lines, lanes),
        out_shape=(shape, shape),
        in_specs=[pl.BlockSpec(memory_space=pltpu.SMEM), whole, whole],
        out_specs=(whole, whole),
        name="block_slots",
    )(device, row_lists[None], panel_cols[None])
    used = (1 + ratio) * lines
    return [slots[:used].reshape(used * lanes) for slots in found]


def one_hot(slot, count, dtype=jnp.float32):
    hot = slot[:, None] == jnp.arange(count, dtype=jnp.int32)
    return hot.astype(jnp.float32).astype(dtype)


def places_kernel(sizes, panel_ref, other_ref, rows_ref, out_ref):
    col_block, ratio, col_slots, col_count = sizes
    row_k = ratio * col_slots
    wide = ratio * row_k
    other = other_ref[...]
    other_home = lax.div(other, jnp.int32(col_block))
    for order in range(2):
        panel = panel_ref[order : order + 1, :]
        home = lax.div(panel, jnp.int32(col_block))
        earlier = (other < panel) & (other_home == home)
        rank = jnp.sum(earlier.astype(jnp.float32), axis=0, keepdims=True).astype(jnp.int32)
        pair = lax.div(home, jnp.int32(ratio))
        place = home - pair * ratio
        out_ref[order : order + 1, :] = home * col_slots + rank
    for part in range(ratio):
        down = pair * wide + part * row_k + place * col_slots + rank
        along = pair * wide + (1 - place) * row_k + part * col_slots + rank
        out_ref[2 + part : 3 + part, :] = down
        out_ref[2 + ratio + part : 3 + ratio + part, :] = along
    out_ref[6:7, :] = rank
    rows_home = lax.div(rows_ref[...], jnp.int32(col_block))
    block = lax.broadcasted_iota(jnp.int32, (col_count, rows_ref.shape[1]), 0)
    counts = jnp.sum((block == rows_home).astype(jnp.float32), axis=1, keepdims=True)
    most = jnp.max(counts, axis=0, keepdims=True).astype(jnp.int32)
    out_ref[7:8, :] = jnp.broadcast_to(most, (1, panel_ref.shape[1]))


def panel_places(col_slots, col_block, ratio, col_count, group, panel_cols, row_lists):
    width = panel_cols.shape[0]
    by_core = jnp.moveaxis(panel_cols.reshape(-1, 2, group), 1, 0).reshape(2, width // 2)
    local = jnp.where(lax.axis_index(COL[1]) == 0, by_core, by_core[::-1]).reshape(width)
    return pl.pallas_call(
        functools.partial(places_kernel, (col_block, ratio, col_slots, col_count)),
        out_shape=jax.ShapeDtypeStruct((8, width), jnp.int32),
        name="panel_places",
    )(jnp.stack([panel_cols, local]), panel_cols[:, None], row_lists[None])


def panel_step(matrix, factor, dinv, panel_cols, row_lists):
    row_count = lax.axis_size(ROW)
    col_count = lax.axis_size(COL)
    ratio = col_count // row_count
    _, col_block = matrix.shape
    width = panel_cols.shape[0]
    dinv_rows = dinv.shape[0]
    row_slots = col_block * 2 // 3
    col_slots = 2 * (width // col_count)
    row_k = ratio * col_slots
    row_pos = lax.axis_index(ROW)
    col_pos = lax.axis_index(COL)
    side = lax.axis_index(COL[1])

    list_slot, panel_slot = block_slots(col_block, ratio, panel_cols, row_lists)
    in_list, in_panel = list_slot >= 0, panel_slot >= 0
    col_in, row_in = in_list[:col_block], in_list[col_block:]
    col_panel, row_panel = in_panel[:col_block], in_panel[col_block:]
    pick = one_hot(list_slot, row_slots)
    pick_cols = pick[:col_block]
    pick_rows = pick[col_block:].reshape(ratio, col_block, row_slots)
    put = one_hot(panel_slot, col_slots)
    put_rows = put[col_block:].reshape(ratio, col_block, col_slots)

    narrow_pick = one_hot(list_slot[:col_block], row_slots, jnp.bfloat16)
    packed = selected(thirds(factor, 1), narrow_pick, BY_FIRST)

    core = lax.axis_index(ROW[2])
    packed = lax.ppermute(packed, (ROW[2], COL[1]), [(0, 0), (1, 2), (2, 1), (3, 3)])
    swap = [(0, 1), (1, 0)]
    copies = jnp.broadcast_to(packed, (lax.axis_size(ROW[:2]), *packed.shape))
    this_block = lax.all_to_all(copies, ROW[:2], 0, 0, tiled=True)
    this_block = this_block.reshape(width // 2, row_slots)
    that_block = lax.ppermute(this_block, ROW[2], swap)
    own_lower = jnp.where(core == side, this_block, that_block)
    pair_lower = jnp.where(core == side, that_block, this_block)

    narrow = dot(matrix, pick_cols).reshape(ratio, col_block, row_slots)
    dense = jnp.stack([dot(pick_rows[part], narrow[part], BY_FIRST) for part in range(ratio)])
    owners = col_count // ratio
    share = row_slots // owners
    dense = jnp.moveaxis(dense.reshape(ratio, owners, share, row_slots), 0, 1)
    dense = dense.reshape(ratio * row_slots, row_slots)
    pair_dense = lax.ppermute(dense, COL[1], swap)

    partial_value = -dot(
        jnp.concatenate([dense, pair_dense], axis=1),
        jnp.concatenate([own_lower, pair_lower], axis=1),
        BY_LAST,
    )
    summed = sum_at_owner(partial_value.reshape(owners, ratio * share, width // 2), COL[0])

    rest_lower = lax.ppermute(pair_lower, COL[1], swap)
    lower = jnp.concatenate([own_lower, rest_lower])

    wide = ratio * row_k
    half_slots = col_slots // 2
    slots = col_count * col_slots
    found = panel_places(
        col_slots, col_block, ratio, col_count, factor.shape[1], panel_cols, row_lists
    )
    slot, local_slot = found[0], found[1]

    def route(places):
        return one_hot(places[:, : width // 2].reshape(-1), row_count * wide, jnp.bfloat16)

    to_rows = route(found[2:4])
    to_cols = route(found[4:6])

    halves_beside = jnp.concatenate([summed[:share], summed[share:]], axis=1)
    parts = thirds(halves_beside, 0)
    chosen = selected(parts, to_rows).reshape(share, row_count, wide)
    received = lax.all_to_all(jnp.moveaxis(chosen, 1, 0), ROW, 0, 0, tiled=True)

    own = jnp.moveaxis(selected(parts, to_cols).reshape(share, row_count, wide), 1, 0)
    lane = jnp.arange(wide, dtype=jnp.int32) // row_k
    sent = jnp.stack([jnp.where(lane == part, received, own) for part in range(ratio)], axis=1)
    arrived = lax.all_to_all(
        sent.reshape(col_count, share, wide), COL, 0, 0, tiled=True
    )
    arrived = jnp.sum(arrived.reshape(owners, ratio, share, wide), axis=1)
    arrived = arrived.reshape(row_slots, wide).T
    upper, under = arrived[:row_k], arrived[row_k:]
    beside = jnp.where(side == 0, upper, under)
    below = jnp.where(side == 0, under, upper)

    def halves(values):
        blocks = values.reshape(col_count, 2, half_slots, values.shape[1])
        return [blocks[:, part].reshape(col_count * half_slots, -1) for part in range(2)]

    lower_slots = dot(one_hot(local_slot, slots), lower, BY_FIRST)
    mine = lax.dynamic_slice_in_dim(slot, col_pos * dinv_rows, dinv_rows)
    placed = dot(
        one_hot(mine, slots), dot(dinv, one_hot(slot - row_pos * row_k, row_k)), BY_FIRST
    )
    lower_pair = jnp.concatenate(halves(lower_slots), axis=1)
    placed_pair = jnp.concatenate(halves(placed), axis=1)
    empty = jnp.zeros_like(beside)
    beside_pair = jnp.concatenate(
        [jnp.concatenate([beside, empty], axis=1), jnp.concatenate([empty, beside], axis=1)]
    )
    terms = placed_pair - dot(lower_pair, beside_pair, BY_LAST)
    corner = sum_at_owner(terms.reshape(col_count, half_slots, 2 * row_k), COL)

    below_rows = [dot(pick_rows[part], below[part * col_slots : (part + 1) * col_slots], BY_LAST) for part in range(ratio)]
    spread_out = dot(beside, pick_cols, BY_LAST)
    at_rows = jnp.concatenate(
        [
            dot(put_rows[part], spread_out[part * col_slots : (part + 1) * col_slots])
            for part in range(ratio)
        ]
    )
    with_rows = jnp.where(row_panel[:, None] & col_in[None, :], at_rows, matrix)
    corner = jnp.concatenate([corner[:, :row_k], corner[:, row_k:]])
    at_cols = jnp.concatenate(
        [
            below_rows[part]
            + dot(
                put_rows[part],
                corner[:, part * col_slots : (part + 1) * col_slots],
                BY_LAST,
            )
            for part in range(ratio)
        ]
    )
    thrice = jnp.concatenate([one_hot(panel_slot[:col_block], col_slots, jnp.bfloat16)] * 3, axis=1)
    at_cols = lax.dot_general(
        thirds(at_cols, 1),
        thrice,
        (BY_LAST, ((), ())),
        preferred_element_type=jnp.float32,
    )
    taken_over = (row_panel | row_in)[:, None] & col_panel[None, :]
    result = jnp.where(taken_over, at_cols, with_rows)

    fits = (jnp.max(found[6]) < col_slots) & (jnp.max(found[7]) <= row_slots)

    def again(carried):
        general = general_panel(matrix, factor, dinv, panel_cols, row_in, col_in)
        return jnp.zeros((), jnp.bool_), general

    return lax.while_loop(lambda carried: carried[0], again, (~fits, result))[1]


def on_device(resident, factor, dinv, panel_cols, row_lists):
    matrix = resident
    for panel in reversed(range(factor.shape[0])):
        matrix = panel_step(matrix, factor[panel], dinv[panel], panel_cols[panel], row_lists[panel])
    return matrix


def solution(mesh):
    finer = Mesh(
        mesh.devices.reshape(-1, 2, 2, mesh.shape["col"] // 2, 2), ROW + COL
    )
    return jax.shard_map(
        on_device,
        mesh=finer,
        in_specs=(P(ROW, COL), P(None, COL, ROW), P(None, COL, None), P(), P()),
        out_specs=P(ROW, COL),
        check_vma=False,
    )
```

```python
import functools

import jax
import jax.numpy as jnp
from jax import lax
from jax.experimental import pallas as pl
from jax.experimental.pallas import tpu as pltpu
from jax.sharding import Mesh
from jax.sharding import PartitionSpec as P


ROW = ("row_0", "row_1", "row_2")
COL = ("col_0", "col_1")
HIGHEST = lax.Precision.HIGHEST
LANES = 128
LINES = 16
BY_LAST = ((1,), (1,))
BY_FIRST = ((0,), (0,))


def dot(a, b, dims=((1,), (0,))):
    return lax.dot_general(
        a, b, (dims, ((), ())), precision=HIGHEST, preferred_element_type=jnp.float32
    )


def thirds(values, axis):
    high = lax.reduce_precision(values, 8, 7)
    rest = values - high
    middle = lax.reduce_precision(rest, 8, 7)
    parts = [part.astype(jnp.bfloat16) for part in (high, middle, rest - middle)]
    return jnp.concatenate(parts, axis=axis)


def selected(parts, hot, dims=((1,), (0,))):
    out = lax.dot_general(
        parts, hot, (dims, ((), ())), preferred_element_type=jnp.float32
    )
    size = out.shape[0] // 3
    return out[:size] + out[size : 2 * size] + out[2 * size :]


def sum_at_owner(blocks, axis):
    return jnp.sum(lax.all_to_all(blocks, axis, 0, 0, tiled=True), axis=0)


def ring_sum(shard, axis):
    count = lax.axis_size(axis)
    ring = [(place, (place + 1) % count) for place in range(count)]

    def step(_, carried):
        moving, total = carried
        moving = lax.ppermute(moving, axis, ring)
        return moving, total + moving

    return lax.fori_loop(0, count - 1, step, (shard, shard))[1]


def general_panel(matrix, factor, dinv, panel_cols, row_in, col_in):
    row_count = lax.axis_size(ROW)
    ratio = lax.axis_size(COL) // row_count
    row_block, col_block = matrix.shape
    width = panel_cols.shape[0]
    group = factor.shape[1]
    row_pos = lax.axis_index(ROW)
    col_pos = lax.axis_index(COL)
    row_ids = row_pos * row_block + jnp.arange(row_block, dtype=jnp.int32)
    col_ids = col_pos * col_block + jnp.arange(col_block, dtype=jnp.int32)
    masked = factor * col_in[:, None].astype(jnp.float32)

    def column_places(turn):
        cols = lax.dynamic_slice_in_dim(panel_cols, turn * group, group)
        return cols, (cols[:, None] == col_ids).astype(jnp.float32)

    def products(turn, carried):
        out, gram = carried
        lower = ring_sum(jnp.where(row_pos == turn, masked, jnp.zeros_like(masked)), ROW)
        by_row = ring_sum(-dot(matrix, lower), COL)
        mine = lax.dynamic_slice_in_dim(by_row, col_pos % ratio * col_block, col_block, 0)
        mine = jnp.where(row_pos == col_pos // ratio, mine, jnp.zeros_like(mine))
        by_col = ring_sum(mine, ROW)
        gram = lax.dynamic_update_slice(
            gram, dot(masked, by_col, BY_FIRST), (row_pos * group, turn * group)
        )
        cols, put_cols = column_places(turn)
        put_rows = (row_ids[:, None] == cols).astype(jnp.float32)
        here = jnp.sum(put_cols, axis=0) > 0.5
        there = jnp.sum(put_rows, axis=1) > 0.5
        out = jnp.where(
            row_in[:, None] & here[None, :],
            dot(by_row, put_cols),
            jnp.where(there[:, None] & col_in[None, :], dot(put_rows, by_col, BY_LAST), out),
        )
        return out, gram

    none = jnp.zeros((width, width), jnp.float32)
    out, gram = lax.fori_loop(0, row_count, products, (matrix, none))
    placed = lax.dynamic_update_slice(none, dinv, (col_pos * dinv.shape[0], 0))
    placed = jnp.where(row_pos == 0, placed, none)
    diagonal = ring_sum(ring_sum(placed - gram, ROW), COL)
    put_rows = (row_ids[:, None] == panel_cols).astype(jnp.float32)
    there = jnp.sum(put_rows, axis=1) > 0.5

    def corners(turn, out):
        _, put_cols = column_places(turn)
        here = jnp.sum(put_cols, axis=0) > 0.5
        part = lax.dynamic_slice_in_dim(diagonal, turn * group, group, 1)
        corner = dot(dot(put_rows, part), put_cols)
        return jnp.where(there[:, None] & here[None, :], corner, out)

    return lax.fori_loop(0, row_count, corners, out)


def slots_kernel(lines, lanes, device_ref, rows_ref, cols_ref, row_slots_ref, col_slots_ref):
    line = lax.broadcasted_iota(jnp.int32, (LINES, 1), 0)
    own = jnp.where(
        line < lines, device_ref[0] * lines + line, device_ref[1] * lines + line - lines
    )
    lower = lax.broadcasted_iota(jnp.int32, (lanes, lanes), 0)
    upper = lax.broadcasted_iota(jnp.int32, (lanes, lanes), 1)
    earlier = (lower < upper).astype(jnp.float32)
    for listed_ref, out_ref in ((rows_ref, row_slots_ref), (cols_ref, col_slots_ref)):
        count = listed_ref.shape[1]
        step = min(count, 1024)
        found = jnp.zeros((LINES, lanes), jnp.float32)
        for start in range(0, count, step):
            size = min(step, count - start)
            listed = listed_ref[:, start : start + size]
            high = lax.div(listed, jnp.int32(lanes))
            low = listed - high * lanes
            line_hit = (own == high).astype(jnp.float32)
            lane_hit = lax.broadcasted_iota(jnp.int32, (lanes, size), 0) == low
            found += lax.dot_general(
                line_hit.astype(jnp.bfloat16),
                lane_hit.astype(jnp.float32).astype(jnp.bfloat16),
                (BY_LAST, ((), ())),
                preferred_element_type=jnp.float32,
            )
        before = jnp.dot(
            found.astype(jnp.bfloat16),
            earlier.astype(jnp.bfloat16),
            preferred_element_type=jnp.float32,
        )
        held = jnp.sum(found, axis=1, keepdims=True)
        for other in range(LINES):
            if (other + 1) % lines:
                later = (line > other) & (line < (other // lines + 1) * lines)
                before += jnp.where(later, held[other : other + 1], 0.0)
        out_ref[...] = jnp.where(found > 0.5, before, -1.0).astype(jnp.int32)


def block_slots(col_block, ratio, panel_cols, row_lists):
    lanes = LANES if col_block % LANES == 0 else col_block
    lines = col_block // lanes
    device = jnp.stack([lax.axis_index(COL), lax.axis_index(ROW) * ratio]).astype(jnp.int32)
    shape = jax.ShapeDtypeStruct((LINES, lanes), jnp.int32)
    whole = pl.BlockSpec(memory_space=pltpu.VMEM)
    found = pl.pallas_call(
        functools.partial(slots_kernel, lines, lanes),
        out_shape=(shape, shape),
        in_specs=[pl.BlockSpec(memory_space=pltpu.SMEM), whole, whole],
        out_specs=(whole, whole),
        name="block_slots",
    )(device, row_lists[None], panel_cols[None])
    used = (1 + ratio) * lines
    return [slots[:used].reshape(used * lanes) for slots in found]


def one_hot(slot, count, dtype=jnp.float32):
    hot = slot[:, None] == jnp.arange(count, dtype=jnp.int32)
    return hot.astype(jnp.float32).astype(dtype)


def places_kernel(sizes, panel_ref, other_ref, rows_ref, out_ref):
    col_block, ratio, col_slots, col_count = sizes
    row_k = ratio * col_slots
    wide = ratio * row_k
    other = other_ref[...]
    other_home = lax.div(other, jnp.int32(col_block))
    for order in range(2):
        panel = panel_ref[order : order + 1, :]
        home = lax.div(panel, jnp.int32(col_block))
        earlier = (other < panel) & (other_home == home)
        rank = jnp.sum(earlier.astype(jnp.float32), axis=0, keepdims=True).astype(jnp.int32)
        pair = lax.div(home, jnp.int32(ratio))
        place = home - pair * ratio
        out_ref[order : order + 1, :] = home * col_slots + rank
    for part in range(ratio):
        down = pair * wide + part * row_k + place * col_slots + rank
        along = pair * wide + (1 - place) * row_k + part * col_slots + rank
        out_ref[2 + part : 3 + part, :] = down
        out_ref[2 + ratio + part : 3 + ratio + part, :] = along
    out_ref[6:7, :] = rank
    rows_home = lax.div(rows_ref[...], jnp.int32(col_block))
    block = lax.broadcasted_iota(jnp.int32, (col_count, rows_ref.shape[1]), 0)
    counts = jnp.sum((block == rows_home).astype(jnp.float32), axis=1, keepdims=True)
    most = jnp.max(counts, axis=0, keepdims=True).astype(jnp.int32)
    out_ref[7:8, :] = jnp.broadcast_to(most, (1, panel_ref.shape[1]))


def panel_places(col_slots, col_block, ratio, col_count, group, panel_cols, row_lists):
    width = panel_cols.shape[0]
    by_core = jnp.moveaxis(panel_cols.reshape(-1, 2, group), 1, 0).reshape(2, width // 2)
    local = jnp.where(lax.axis_index(COL[1]) == 0, by_core, by_core[::-1]).reshape(width)
    return pl.pallas_call(
        functools.partial(places_kernel, (col_block, ratio, col_slots, col_count)),
        out_shape=jax.ShapeDtypeStruct((8, width), jnp.int32),
        name="panel_places",
    )(jnp.stack([panel_cols, local]), panel_cols[:, None], row_lists[None])


def panel_step(matrix, factor, dinv, panel_cols, row_lists):
    row_count = lax.axis_size(ROW)
    col_count = lax.axis_size(COL)
    ratio = col_count // row_count
    _, col_block = matrix.shape
    width = panel_cols.shape[0]
    dinv_rows = dinv.shape[0]
    row_slots = col_block * 2 // 3
    col_slots = 2 * (width // col_count)
    row_k = ratio * col_slots
    row_pos = lax.axis_index(ROW)
    col_pos = lax.axis_index(COL)
    side = lax.axis_index(COL[1])

    list_slot, panel_slot = block_slots(col_block, ratio, panel_cols, row_lists)
    in_list, in_panel = list_slot >= 0, panel_slot >= 0
    col_in, row_in = in_list[:col_block], in_list[col_block:]
    col_panel, row_panel = in_panel[:col_block], in_panel[col_block:]
    pick = one_hot(list_slot, row_slots)
    pick_cols = pick[:col_block]
    pick_rows = pick[col_block:].reshape(ratio, col_block, row_slots)
    put = one_hot(panel_slot, col_slots)
    put_rows = put[col_block:].reshape(ratio, col_block, col_slots)

    narrow_pick = one_hot(list_slot[:col_block], row_slots, jnp.bfloat16)
    packed = selected(thirds(factor, 1), narrow_pick, BY_FIRST)

    core = lax.axis_index(ROW[2])
    swap = [(0, 1), (1, 0)]
    copies = jnp.broadcast_to(packed, (lax.axis_size(ROW[:2]), *packed.shape))
    this_half = lax.all_to_all(copies, ROW[:2], 0, 0, tiled=True)
    this_half = this_half.reshape(width // 2, row_slots)
    pair_axes = (ROW[2], COL[1])
    near = lax.ppermute(this_half, pair_axes, [(1, 0), (2, 3)])
    across = lax.ppermute(this_half, pair_axes, [(1, 2), (2, 1)])
    that_half = lax.ppermute(this_half, ROW[2], swap)
    same = core == side
    own_lower = jnp.where(same, this_half, that_half)
    lower = jnp.concatenate([own_lower, jnp.where(same, that_half, this_half)])
    pair_lower = jnp.where(same, near, across)

    narrow = dot(matrix, pick_cols).reshape(ratio, col_block, row_slots)
    dense = jnp.stack([dot(pick_rows[part], narrow[part], BY_FIRST) for part in range(ratio)])
    owners = col_count // ratio
    share = row_slots // owners
    dense = jnp.moveaxis(dense.reshape(ratio, owners, share, row_slots), 0, 1)
    dense = dense.reshape(ratio * row_slots, row_slots)
    pair_dense = lax.ppermute(dense, COL[1], swap)

    partial_value = -dot(
        jnp.concatenate([dense, pair_dense], axis=1),
        jnp.concatenate([own_lower, pair_lower], axis=1),
        BY_LAST,
    )
    summed = sum_at_owner(partial_value.reshape(owners, ratio * share, width // 2), COL[0])

    wide = ratio * row_k
    half_slots = col_slots // 2
    slots = col_count * col_slots
    found = panel_places(
        col_slots, col_block, ratio, col_count, factor.shape[1], panel_cols, row_lists
    )
    slot, local_slot = found[0], found[1]

    def route(places):
        return one_hot(places[:, : width // 2].reshape(-1), row_count * wide, jnp.bfloat16)

    to_rows = route(found[2:4])
    to_cols = route(found[4:6])

    halves_beside = jnp.concatenate([summed[:share], summed[share:]], axis=1)
    parts = thirds(halves_beside, 0)
    chosen = selected(parts, to_rows).reshape(share, row_count, wide)
    received = lax.all_to_all(jnp.moveaxis(chosen, 1, 0), ROW, 0, 0, tiled=True)

    own = jnp.moveaxis(selected(parts, to_cols).reshape(share, row_count, wide), 1, 0)
    lane = jnp.arange(wide, dtype=jnp.int32) // row_k
    sent = jnp.stack([jnp.where(lane == part, received, own) for part in range(ratio)], axis=1)
    arrived = lax.all_to_all(
        sent.reshape(col_count, share, wide), COL, 0, 0, tiled=True
    )
    arrived = jnp.sum(arrived.reshape(owners, ratio, share, wide), axis=1)
    arrived = arrived.reshape(row_slots, wide).T
    upper, under = arrived[:row_k], arrived[row_k:]
    beside = jnp.where(side == 0, upper, under)
    below = jnp.where(side == 0, under, upper)

    def halves(values):
        blocks = values.reshape(col_count, 2, half_slots, values.shape[1])
        return [blocks[:, part].reshape(col_count * half_slots, -1) for part in range(2)]

    lower_slots = dot(one_hot(local_slot, slots), lower, BY_FIRST)
    mine = lax.dynamic_slice_in_dim(slot, col_pos * dinv_rows, dinv_rows)
    placed = dot(
        one_hot(mine, slots), dot(dinv, one_hot(slot - row_pos * row_k, row_k)), BY_FIRST
    )
    lower_pair = jnp.concatenate(halves(lower_slots), axis=1)
    placed_pair = jnp.concatenate(halves(placed), axis=1)
    empty = jnp.zeros_like(beside)
    beside_pair = jnp.concatenate(
        [jnp.concatenate([beside, empty], axis=1), jnp.concatenate([empty, beside], axis=1)]
    )
    terms = placed_pair - dot(lower_pair, beside_pair, BY_LAST)
    corner = sum_at_owner(terms.reshape(col_count, half_slots, 2 * row_k), COL)

    below_rows = [dot(pick_rows[part], below[part * col_slots : (part + 1) * col_slots], BY_LAST) for part in range(ratio)]
    spread_out = dot(beside, pick_cols, BY_LAST)
    at_rows = jnp.concatenate(
        [
            dot(put_rows[part], spread_out[part * col_slots : (part + 1) * col_slots])
            for part in range(ratio)
        ]
    )
    with_rows = jnp.where(row_panel[:, None] & col_in[None, :], at_rows, matrix)
    corner = jnp.concatenate([corner[:, :row_k], corner[:, row_k:]])
    at_cols = jnp.concatenate(
        [
            below_rows[part]
            + dot(
                put_rows[part],
                corner[:, part * col_slots : (part + 1) * col_slots],
                BY_LAST,
            )
            for part in range(ratio)
        ]
    )
    thrice = jnp.concatenate([one_hot(panel_slot[:col_block], col_slots, jnp.bfloat16)] * 3, axis=1)
    at_cols = lax.dot_general(
        thirds(at_cols, 1),
        thrice,
        (BY_LAST, ((), ())),
        preferred_element_type=jnp.float32,
    )
    taken_over = (row_panel | row_in)[:, None] & col_panel[None, :]
    result = jnp.where(taken_over, at_cols, with_rows)

    fits = (jnp.max(found[6]) < col_slots) & (jnp.max(found[7]) <= row_slots)

    def again(carried):
        general = general_panel(matrix, factor, dinv, panel_cols, row_in, col_in)
        return jnp.zeros((), jnp.bool_), general

    return lax.while_loop(lambda carried: carried[0], again, (~fits, result))[1]


def on_device(resident, factor, dinv, panel_cols, row_lists):
    matrix = resident
    for panel in reversed(range(factor.shape[0])):
        matrix = panel_step(matrix, factor[panel], dinv[panel], panel_cols[panel], row_lists[panel])
    return matrix


def solution(mesh):
    finer = Mesh(
        mesh.devices.reshape(-1, 2, 2, mesh.shape["col"] // 2, 2), ROW + COL
    )
    return jax.shard_map(
        on_device,
        mesh=finer,
        in_specs=(P(ROW, COL), P(None, COL, ROW), P(None, COL, None), P(), P()),
        out_specs=P(ROW, COL),
        check_vma=False,
    )
```

```python
import functools

import jax
import jax.numpy as jnp
from jax import lax
from jax.experimental import pallas as pl
from jax.experimental.pallas import tpu as pltpu
from jax.sharding import Mesh
from jax.sharding import PartitionSpec as P


ROW = ("row_0", "row_1", "row_2")
COL = ("col_0", "col_1")
HIGHEST = lax.Precision.HIGHEST
LANES = 128
LINES = 16
BY_LAST = ((1,), (1,))
BY_FIRST = ((0,), (0,))


def dot(a, b, dims=((1,), (0,))):
    return lax.dot_general(
        a, b, (dims, ((), ())), precision=HIGHEST, preferred_element_type=jnp.float32
    )


def thirds(values, axis):
    high = lax.reduce_precision(values, 8, 7)
    rest = values - high
    middle = lax.reduce_precision(rest, 8, 7)
    parts = [part.astype(jnp.bfloat16) for part in (high, middle, rest - middle)]
    return jnp.concatenate(parts, axis=axis)


def selected(parts, hot, dims=((1,), (0,))):
    out = lax.dot_general(
        parts, hot, (dims, ((), ())), preferred_element_type=jnp.float32
    )
    size = out.shape[0] // 3
    return out[:size] + out[size : 2 * size] + out[2 * size :]


def sum_at_owner(blocks, axis):
    return jnp.sum(lax.all_to_all(blocks, axis, 0, 0, tiled=True), axis=0)


def ring_sum(shard, axis):
    count = lax.axis_size(axis)
    ring = [(place, (place + 1) % count) for place in range(count)]

    def step(_, carried):
        moving, total = carried
        moving = lax.ppermute(moving, axis, ring)
        return moving, total + moving

    return lax.fori_loop(0, count - 1, step, (shard, shard))[1]


def general_panel(matrix, factor, dinv, panel_cols, row_in, col_in):
    row_count = lax.axis_size(ROW)
    ratio = lax.axis_size(COL) // row_count
    row_block, col_block = matrix.shape
    width = panel_cols.shape[0]
    group = factor.shape[1]
    row_pos = lax.axis_index(ROW)
    col_pos = lax.axis_index(COL)
    row_ids = row_pos * row_block + jnp.arange(row_block, dtype=jnp.int32)
    col_ids = col_pos * col_block + jnp.arange(col_block, dtype=jnp.int32)
    masked = factor * col_in[:, None].astype(jnp.float32)

    def column_places(turn):
        cols = lax.dynamic_slice_in_dim(panel_cols, turn * group, group)
        return cols, (cols[:, None] == col_ids).astype(jnp.float32)

    def products(turn, carried):
        out, gram = carried
        lower = ring_sum(jnp.where(row_pos == turn, masked, jnp.zeros_like(masked)), ROW)
        by_row = ring_sum(-dot(matrix, lower), COL)
        mine = lax.dynamic_slice_in_dim(by_row, col_pos % ratio * col_block, col_block, 0)
        mine = jnp.where(row_pos == col_pos // ratio, mine, jnp.zeros_like(mine))
        by_col = ring_sum(mine, ROW)
        gram = lax.dynamic_update_slice(
            gram, dot(masked, by_col, BY_FIRST), (row_pos * group, turn * group)
        )
        cols, put_cols = column_places(turn)
        put_rows = (row_ids[:, None] == cols).astype(jnp.float32)
        here = jnp.sum(put_cols, axis=0) > 0.5
        there = jnp.sum(put_rows, axis=1) > 0.5
        out = jnp.where(
            row_in[:, None] & here[None, :],
            dot(by_row, put_cols),
            jnp.where(there[:, None] & col_in[None, :], dot(put_rows, by_col, BY_LAST), out),
        )
        return out, gram

    none = jnp.zeros((width, width), jnp.float32)
    out, gram = lax.fori_loop(0, row_count, products, (matrix, none))
    placed = lax.dynamic_update_slice(none, dinv, (col_pos * dinv.shape[0], 0))
    placed = jnp.where(row_pos == 0, placed, none)
    diagonal = ring_sum(ring_sum(placed - gram, ROW), COL)
    put_rows = (row_ids[:, None] == panel_cols).astype(jnp.float32)
    there = jnp.sum(put_rows, axis=1) > 0.5

    def corners(turn, out):
        _, put_cols = column_places(turn)
        here = jnp.sum(put_cols, axis=0) > 0.5
        part = lax.dynamic_slice_in_dim(diagonal, turn * group, group, 1)
        corner = dot(dot(put_rows, part), put_cols)
        return jnp.where(there[:, None] & here[None, :], corner, out)

    return lax.fori_loop(0, row_count, corners, out)


def slots_kernel(lines, lanes, ratio, rows_ref, cols_ref, row_slots_ref, col_slots_ref):
    line = lax.broadcasted_iota(jnp.int32, (LINES, 1), 0)
    own = jnp.where(
        line < lines,
        lax.axis_index(COL) * lines + line,
        (lax.axis_index(ROW) * ratio - 1) * lines + line,
    )
    lower = lax.broadcasted_iota(jnp.int32, (lanes, lanes), 0)
    upper = lax.broadcasted_iota(jnp.int32, (lanes, lanes), 1)
    earlier = (lower < upper).astype(jnp.float32)
    for listed_ref, out_ref in ((rows_ref, row_slots_ref), (cols_ref, col_slots_ref)):
        count = listed_ref.shape[1]
        step = min(count, 1024)
        found = jnp.zeros((LINES, lanes), jnp.float32)
        for start in range(0, count, step):
            size = min(step, count - start)
            listed = listed_ref[:, start : start + size]
            high = lax.div(listed, jnp.int32(lanes))
            low = listed - high * lanes
            line_hit = (own == high).astype(jnp.float32)
            lane_hit = lax.broadcasted_iota(jnp.int32, (lanes, size), 0) == low
            found += lax.dot_general(
                line_hit.astype(jnp.bfloat16),
                lane_hit.astype(jnp.float32).astype(jnp.bfloat16),
                (BY_LAST, ((), ())),
                preferred_element_type=jnp.float32,
            )
        before = jnp.dot(
            found.astype(jnp.bfloat16),
            earlier.astype(jnp.bfloat16),
            preferred_element_type=jnp.float32,
        )
        held = jnp.sum(found, axis=1, keepdims=True)
        for other in range(LINES):
            if (other + 1) % lines:
                later = (line > other) & (line < (other // lines + 1) * lines)
                before += jnp.where(later, held[other : other + 1], 0.0)
        out_ref[...] = jnp.where(found > 0.5, before, -1.0).astype(jnp.int32)


def block_slots(col_block, ratio, panel_cols, row_lists):
    lanes = LANES if col_block % LANES == 0 else col_block
    lines = col_block // lanes
    shape = jax.ShapeDtypeStruct((LINES, lanes), jnp.int32)
    whole = pl.BlockSpec(memory_space=pltpu.VMEM)
    found = pl.pallas_call(
        functools.partial(slots_kernel, lines, lanes, ratio),
        out_shape=(shape, shape),
        in_specs=[whole, whole],
        out_specs=(whole, whole),
        name="block_slots",
    )(row_lists[None], panel_cols[None])
    used = (1 + ratio) * lines
    return [slots[:used].reshape(used * lanes) for slots in found]


def one_hot(slot, count, dtype=jnp.float32):
    hot = slot[:, None] == jnp.arange(count, dtype=jnp.int32)
    return hot.astype(jnp.float32).astype(dtype)


def places_kernel(sizes, own_ref, local_ref, rows_ref, out_ref):
    col_block, ratio, col_slots, col_count = sizes
    row_k = ratio * col_slots
    wide = ratio * row_k
    width = own_ref.shape[1]
    other = jnp.broadcast_to(own_ref[...].astype(jnp.float32), (8, width)).T[:, :1]
    other = other.astype(jnp.int32)
    other_home = lax.div(other, jnp.int32(col_block))
    for order, panel_ref in enumerate((own_ref, local_ref)):
        panel = panel_ref[...]
        home = lax.div(panel, jnp.int32(col_block))
        earlier = (other < panel) & (other_home == home)
        rank = jnp.sum(earlier.astype(jnp.float32), axis=0, keepdims=True).astype(jnp.int32)
        pair = lax.div(home, jnp.int32(ratio))
        place = home - pair * ratio
        out_ref[order : order + 1, :] = home * col_slots + rank
    for part in range(ratio):
        down = pair * wide + part * row_k + place * col_slots + rank
        along = pair * wide + (1 - place) * row_k + part * col_slots + rank
        out_ref[2 + part : 3 + part, :] = down
        out_ref[2 + ratio + part : 3 + ratio + part, :] = along
    out_ref[6:7, :] = rank
    rows_home = lax.div(rows_ref[...], jnp.int32(col_block))
    block = lax.broadcasted_iota(jnp.int32, (col_count, rows_ref.shape[1]), 0)
    counts = jnp.sum((block == rows_home).astype(jnp.float32), axis=1, keepdims=True)
    most = jnp.max(counts, axis=0, keepdims=True).astype(jnp.int32)
    out_ref[7:8, :] = jnp.broadcast_to(most, (1, width))


def panel_places(col_slots, col_block, ratio, col_count, group, panel_cols, row_lists):
    width = panel_cols.shape[0]
    by_core = jnp.moveaxis(panel_cols.reshape(-1, 2, group), 1, 0).reshape(2, width // 2)
    local = jnp.where(lax.axis_index(COL[1]) == 0, by_core, by_core[::-1]).reshape(width)
    return pl.pallas_call(
        functools.partial(places_kernel, (col_block, ratio, col_slots, col_count)),
        out_shape=jax.ShapeDtypeStruct((8, width), jnp.int32),
        name="panel_places",
    )(panel_cols[None], local[None], row_lists[None])


def panel_step(matrix, factor, dinv, panel_cols, row_lists):
    row_count = lax.axis_size(ROW)
    col_count = lax.axis_size(COL)
    ratio = col_count // row_count
    _, col_block = matrix.shape
    width = panel_cols.shape[0]
    dinv_rows = dinv.shape[0]
    row_slots = col_block * 2 // 3
    col_slots = 2 * (width // col_count)
    row_k = ratio * col_slots
    row_pos = lax.axis_index(ROW)
    col_pos = lax.axis_index(COL)
    side = lax.axis_index(COL[1])

    list_slot, panel_slot = block_slots(col_block, ratio, panel_cols, row_lists)
    in_list, in_panel = list_slot >= 0, panel_slot >= 0
    col_in, row_in = in_list[:col_block], in_list[col_block:]
    col_panel, row_panel = in_panel[:col_block], in_panel[col_block:]
    pick = one_hot(list_slot, row_slots)
    pick_cols = pick[:col_block]
    pick_rows = pick[col_block:].reshape(ratio, col_block, row_slots)
    put = one_hot(panel_slot, col_slots)
    put_rows = put[col_block:].reshape(ratio, col_block, col_slots)

    narrow_pick = one_hot(list_slot[:col_block], row_slots, jnp.bfloat16)
    packed = selected(thirds(factor, 1), narrow_pick, BY_FIRST)

    core = lax.axis_index(ROW[2])
    swap = [(0, 1), (1, 0)]
    copies = jnp.broadcast_to(packed, (lax.axis_size(ROW[:2]), *packed.shape))
    this_half = lax.all_to_all(copies, ROW[:2], 0, 0, tiled=True)
    this_half = this_half.reshape(width // 2, row_slots)
    pair_axes = (ROW[2], COL[1])
    near = lax.ppermute(this_half, pair_axes, [(1, 0), (2, 3)])
    across = lax.ppermute(this_half, pair_axes, [(1, 2), (2, 1)])
    that_half = lax.ppermute(this_half, ROW[2], swap)
    same = core == side
    own_lower = jnp.where(same, this_half, that_half)
    lower = jnp.concatenate([own_lower, jnp.where(same, that_half, this_half)])
    pair_lower = jnp.where(same, near, across)

    narrow = dot(matrix, pick_cols).reshape(ratio, col_block, row_slots)
    dense = jnp.stack([dot(pick_rows[part], narrow[part], BY_FIRST) for part in range(ratio)])
    owners = col_count // ratio
    share = row_slots // owners
    dense = jnp.moveaxis(dense.reshape(ratio, owners, share, row_slots), 0, 1)
    dense = dense.reshape(ratio * row_slots, row_slots)
    pair_dense = lax.ppermute(dense, COL[1], swap)

    partial_value = -dot(
        jnp.concatenate([dense, pair_dense], axis=1),
        jnp.concatenate([own_lower, pair_lower], axis=1),
        BY_LAST,
    )
    summed = sum_at_owner(partial_value.reshape(owners, ratio * share, width // 2), COL[0])

    wide = ratio * row_k
    half_slots = col_slots // 2
    slots = col_count * col_slots
    found = panel_places(
        col_slots, col_block, ratio, col_count, factor.shape[1], panel_cols, row_lists
    )
    slot, local_slot = found[0], found[1]

    def route(places):
        return one_hot(places[:, : width // 2].reshape(-1), row_count * wide, jnp.bfloat16)

    to_rows = route(found[2:4])
    to_cols = route(found[4:6])

    halves_beside = jnp.concatenate([summed[:share], summed[share:]], axis=1)
    parts = thirds(halves_beside, 0)
    chosen = selected(parts, to_rows).reshape(share, row_count, wide)
    received = lax.all_to_all(jnp.moveaxis(chosen, 1, 0), ROW, 0, 0, tiled=True)

    own = jnp.moveaxis(selected(parts, to_cols).reshape(share, row_count, wide), 1, 0)
    lane = jnp.arange(wide, dtype=jnp.int32) // row_k
    sent = jnp.stack([jnp.where(lane == part, received, own) for part in range(ratio)], axis=1)
    arrived = lax.all_to_all(
        sent.reshape(col_count, share, wide), COL, 0, 0, tiled=True
    )
    arrived = jnp.sum(arrived.reshape(owners, ratio, share, wide), axis=1)
    arrived = arrived.reshape(row_slots, wide).T
    upper, under = arrived[:row_k], arrived[row_k:]
    beside = jnp.where(side == 0, upper, under)
    below = jnp.where(side == 0, under, upper)

    def halves(values):
        blocks = values.reshape(col_count, 2, half_slots, values.shape[1])
        return [blocks[:, part].reshape(col_count * half_slots, -1) for part in range(2)]

    lower_slots = dot(one_hot(local_slot, slots), lower, BY_FIRST)
    mine = lax.dynamic_slice_in_dim(slot, col_pos * dinv_rows, dinv_rows)
    placed = dot(
        one_hot(mine, slots), dot(dinv, one_hot(slot - row_pos * row_k, row_k)), BY_FIRST
    )
    lower_pair = jnp.concatenate(halves(lower_slots), axis=1)
    placed_pair = jnp.concatenate(halves(placed), axis=1)
    empty = jnp.zeros_like(beside)
    beside_pair = jnp.concatenate(
        [jnp.concatenate([beside, empty], axis=1), jnp.concatenate([empty, beside], axis=1)]
    )
    terms = placed_pair - dot(lower_pair, beside_pair, BY_LAST)
    corner = sum_at_owner(terms.reshape(col_count, half_slots, 2 * row_k), COL)

    below_rows = [dot(pick_rows[part], below[part * col_slots : (part + 1) * col_slots], BY_LAST) for part in range(ratio)]
    spread_out = dot(beside, pick_cols, BY_LAST)
    at_rows = jnp.concatenate(
        [
            dot(put_rows[part], spread_out[part * col_slots : (part + 1) * col_slots])
            for part in range(ratio)
        ]
    )
    with_rows = jnp.where(row_panel[:, None] & col_in[None, :], at_rows, matrix)
    corner = jnp.concatenate([corner[:, :row_k], corner[:, row_k:]])
    at_cols = jnp.concatenate(
        [
            below_rows[part]
            + dot(
                put_rows[part],
                corner[:, part * col_slots : (part + 1) * col_slots],
                BY_LAST,
            )
            for part in range(ratio)
        ]
    )
    thrice = jnp.concatenate([one_hot(panel_slot[:col_block], col_slots, jnp.bfloat16)] * 3, axis=1)
    at_cols = lax.dot_general(
        thirds(at_cols, 1),
        thrice,
        (BY_LAST, ((), ())),
        preferred_element_type=jnp.float32,
    )
    taken_over = (row_panel | row_in)[:, None] & col_panel[None, :]
    result = jnp.where(taken_over, at_cols, with_rows)

    fits = (jnp.max(found[6]) < col_slots) & (jnp.max(found[7]) <= row_slots)

    zero = lax.shift_right_logical((received[0, 0, 0] > 0.0).astype(jnp.int32), 1)
    late_factor = factor + zero.astype(jnp.float32)
    late_dinv = dinv + zero.astype(jnp.float32)

    def again(carried):
        general = general_panel(matrix, late_factor, late_dinv, panel_cols, row_in, col_in)
        return jnp.zeros((), jnp.bool_), general

    return lax.while_loop(lambda carried: carried[0], again, (~fits, result))[1]


def on_device(resident, factor, dinv, panel_cols, row_lists):
    matrix = resident
    for panel in reversed(range(factor.shape[0])):
        matrix = panel_step(matrix, factor[panel], dinv[panel], panel_cols[panel], row_lists[panel])
    return matrix


def solution(mesh):
    finer = Mesh(
        mesh.devices.reshape(-1, 2, 2, mesh.shape["col"] // 2, 2), ROW + COL
    )
    return jax.shard_map(
        on_device,
        mesh=finer,
        in_specs=(P(ROW, COL), P(None, COL, ROW), P(None, COL, None), P(), P()),
        out_specs=P(ROW, COL),
        check_vma=False,
    )
```

```python
import functools

import jax
import jax.numpy as jnp
from jax import lax
from jax.experimental import pallas as pl
from jax.experimental.pallas import tpu as pltpu
from jax.sharding import Mesh
from jax.sharding import PartitionSpec as P


ROW = ("row_0", "row_1", "row_2")
COL = ("col_0", "col_1")
HIGHEST = lax.Precision.HIGHEST
LANES = 128
LINES = 16
BY_LAST = ((1,), (1,))
BY_FIRST = ((0,), (0,))


def dot(a, b, dims=((1,), (0,))):
    return lax.dot_general(
        a, b, (dims, ((), ())), precision=HIGHEST, preferred_element_type=jnp.float32
    )


def thirds(values, axis):
    high = lax.reduce_precision(values, 8, 7)
    rest = values - high
    middle = lax.reduce_precision(rest, 8, 7)
    parts = [part.astype(jnp.bfloat16) for part in (high, middle, rest - middle)]
    return jnp.concatenate(parts, axis=axis)


def selected(parts, hot, dims=((1,), (0,))):
    out = lax.dot_general(
        parts, hot, (dims, ((), ())), preferred_element_type=jnp.float32
    )
    size = out.shape[0] // 3
    return out[:size] + out[size : 2 * size] + out[2 * size :]


def sum_at_owner(blocks, axis):
    return jnp.sum(lax.all_to_all(blocks, axis, 0, 0, tiled=True), axis=0)


def ring_sum(shard, axis):
    count = lax.axis_size(axis)
    ring = [(place, (place + 1) % count) for place in range(count)]

    def step(_, carried):
        moving, total = carried
        moving = lax.ppermute(moving, axis, ring)
        return moving, total + moving

    return lax.fori_loop(0, count - 1, step, (shard, shard))[1]


def general_panel(matrix, factor, dinv, panel_cols, row_in, col_in):
    row_count = lax.axis_size(ROW)
    ratio = lax.axis_size(COL) // row_count
    row_block, col_block = matrix.shape
    width = panel_cols.shape[0]
    group = factor.shape[1]
    row_pos = lax.axis_index(ROW)
    col_pos = lax.axis_index(COL)
    row_ids = row_pos * row_block + jnp.arange(row_block, dtype=jnp.int32)
    col_ids = col_pos * col_block + jnp.arange(col_block, dtype=jnp.int32)
    masked = factor * col_in[:, None].astype(jnp.float32)

    def column_places(turn):
        cols = lax.dynamic_slice_in_dim(panel_cols, turn * group, group)
        return cols, (cols[:, None] == col_ids).astype(jnp.float32)

    def products(turn, carried):
        out, gram = carried
        lower = ring_sum(jnp.where(row_pos == turn, masked, jnp.zeros_like(masked)), ROW)
        by_row = ring_sum(-dot(matrix, lower), COL)
        mine = lax.dynamic_slice_in_dim(by_row, col_pos % ratio * col_block, col_block, 0)
        mine = jnp.where(row_pos == col_pos // ratio, mine, jnp.zeros_like(mine))
        by_col = ring_sum(mine, ROW)
        gram = lax.dynamic_update_slice(
            gram, dot(masked, by_col, BY_FIRST), (row_pos * group, turn * group)
        )
        cols, put_cols = column_places(turn)
        put_rows = (row_ids[:, None] == cols).astype(jnp.float32)
        here = jnp.sum(put_cols, axis=0) > 0.5
        there = jnp.sum(put_rows, axis=1) > 0.5
        out = jnp.where(
            row_in[:, None] & here[None, :],
            dot(by_row, put_cols),
            jnp.where(there[:, None] & col_in[None, :], dot(put_rows, by_col, BY_LAST), out),
        )
        return out, gram

    none = jnp.zeros((width, width), jnp.float32)
    out, gram = lax.fori_loop(0, row_count, products, (matrix, none))
    placed = lax.dynamic_update_slice(none, dinv, (col_pos * dinv.shape[0], 0))
    placed = jnp.where(row_pos == 0, placed, none)
    diagonal = ring_sum(ring_sum(placed - gram, ROW), COL)
    put_rows = (row_ids[:, None] == panel_cols).astype(jnp.float32)
    there = jnp.sum(put_rows, axis=1) > 0.5

    def corners(turn, out):
        _, put_cols = column_places(turn)
        here = jnp.sum(put_cols, axis=0) > 0.5
        part = lax.dynamic_slice_in_dim(diagonal, turn * group, group, 1)
        corner = dot(dot(put_rows, part), put_cols)
        return jnp.where(there[:, None] & here[None, :], corner, out)

    return lax.fori_loop(0, row_count, corners, out)


def slots_kernel(lines, lanes, ratio, rows_ref, cols_ref, row_slots_ref, col_slots_ref):
    line = lax.broadcasted_iota(jnp.int32, (LINES, 1), 0)
    own = jnp.where(
        line < lines,
        lax.axis_index(COL) * lines + line,
        (lax.axis_index(ROW) * ratio - 1) * lines + line,
    )
    lower = lax.broadcasted_iota(jnp.int32, (lanes, lanes), 0)
    upper = lax.broadcasted_iota(jnp.int32, (lanes, lanes), 1)
    earlier = (lower < upper).astype(jnp.float32)
    for listed_ref, out_ref in ((rows_ref, row_slots_ref), (cols_ref, col_slots_ref)):
        count = listed_ref.shape[1]
        step = min(count, 1024)
        found = jnp.zeros((LINES, lanes), jnp.float32)
        for start in range(0, count, step):
            size = min(step, count - start)
            listed = listed_ref[:, start : start + size]
            high = lax.div(listed, jnp.int32(lanes))
            low = listed - high * lanes
            line_hit = (own == high).astype(jnp.float32)
            lane_hit = lax.broadcasted_iota(jnp.int32, (lanes, size), 0) == low
            found += lax.dot_general(
                line_hit.astype(jnp.bfloat16),
                lane_hit.astype(jnp.float32).astype(jnp.bfloat16),
                (BY_LAST, ((), ())),
                preferred_element_type=jnp.float32,
            )
        before = jnp.dot(
            found.astype(jnp.bfloat16),
            earlier.astype(jnp.bfloat16),
            preferred_element_type=jnp.float32,
        )
        held = jnp.sum(found, axis=1, keepdims=True)
        for other in range(LINES):
            if (other + 1) % lines:
                later = (line > other) & (line < (other // lines + 1) * lines)
                before += jnp.where(later, held[other : other + 1], 0.0)
        out_ref[...] = jnp.where(found > 0.5, before, -1.0).astype(jnp.int32)


def block_slots(col_block, ratio, panel_cols, row_lists):
    lanes = LANES if col_block % LANES == 0 else col_block
    lines = col_block // lanes
    shape = jax.ShapeDtypeStruct((LINES, lanes), jnp.int32)
    whole = pl.BlockSpec(memory_space=pltpu.VMEM)
    found = pl.pallas_call(
        functools.partial(slots_kernel, lines, lanes, ratio),
        out_shape=(shape, shape),
        in_specs=[whole, whole],
        out_specs=(whole, whole),
        name="block_slots",
    )(row_lists[None], panel_cols[None])
    used = (1 + ratio) * lines
    return [slots[:used].reshape(used * lanes) for slots in found]


def one_hot(slot, count, dtype=jnp.float32):
    hot = slot[:, None] == jnp.arange(count, dtype=jnp.int32)
    return hot.astype(jnp.float32).astype(dtype)


def places_kernel(sizes, own_ref, local_ref, rows_ref, out_ref):
    col_block, ratio, col_slots, col_count = sizes
    row_k = ratio * col_slots
    wide = ratio * row_k
    width = own_ref.shape[1]
    other = jnp.broadcast_to(own_ref[...].astype(jnp.float32), (8, width)).T[:, :1]
    other = other.astype(jnp.int32)
    other_home = lax.div(other, jnp.int32(col_block))
    for order, panel_ref in enumerate((own_ref, local_ref)):
        panel = panel_ref[...]
        home = lax.div(panel, jnp.int32(col_block))
        earlier = (other < panel) & (other_home == home)
        rank = jnp.sum(earlier.astype(jnp.float32), axis=0, keepdims=True).astype(jnp.int32)
        pair = lax.div(home, jnp.int32(ratio))
        place = home - pair * ratio
        out_ref[order : order + 1, :] = home * col_slots + rank
    for part in range(ratio):
        down = pair * wide + part * row_k + place * col_slots + rank
        along = pair * wide + (1 - place) * row_k + part * col_slots + rank
        out_ref[2 + part : 3 + part, :] = down
        out_ref[2 + ratio + part : 3 + ratio + part, :] = along
    out_ref[6:7, :] = rank
    rows_home = lax.div(rows_ref[...], jnp.int32(col_block))
    block = lax.broadcasted_iota(jnp.int32, (col_count, rows_ref.shape[1]), 0)
    counts = jnp.sum((block == rows_home).astype(jnp.float32), axis=1, keepdims=True)
    most = jnp.max(counts, axis=0, keepdims=True).astype(jnp.int32)
    out_ref[7:8, :] = jnp.broadcast_to(most, (1, width))


def panel_places(col_slots, col_block, ratio, col_count, group, panel_cols, row_lists):
    width = panel_cols.shape[0]
    by_core = jnp.moveaxis(panel_cols.reshape(-1, 2, group), 1, 0).reshape(2, width // 2)
    local = jnp.where(lax.axis_index(ROW[2]) == 0, by_core, by_core[::-1]).reshape(width)
    return pl.pallas_call(
        functools.partial(places_kernel, (col_block, ratio, col_slots, col_count)),
        out_shape=jax.ShapeDtypeStruct((8, width), jnp.int32),
        name="panel_places",
    )(panel_cols[None], local[None], row_lists[None])


def panel_step(matrix, factor, dinv, panel_cols, row_lists):
    row_count = lax.axis_size(ROW)
    col_count = lax.axis_size(COL)
    ratio = col_count // row_count
    _, col_block = matrix.shape
    width = panel_cols.shape[0]
    dinv_rows = dinv.shape[0]
    row_slots = col_block * 2 // 3
    col_slots = 2 * (width // col_count)
    row_k = ratio * col_slots
    row_pos = lax.axis_index(ROW)
    col_pos = lax.axis_index(COL)
    side = lax.axis_index(COL[1])

    list_slot, panel_slot = block_slots(col_block, ratio, panel_cols, row_lists)
    in_list, in_panel = list_slot >= 0, panel_slot >= 0
    col_in, row_in = in_list[:col_block], in_list[col_block:]
    col_panel, row_panel = in_panel[:col_block], in_panel[col_block:]
    pick = one_hot(list_slot, row_slots)
    pick_cols = pick[:col_block]
    pick_rows = pick[col_block:].reshape(ratio, col_block, row_slots)
    put = one_hot(panel_slot, col_slots)
    put_rows = put[col_block:].reshape(ratio, col_block, col_slots)

    narrow_pick = one_hot(list_slot[:col_block], row_slots, jnp.bfloat16)
    packed = selected(thirds(factor, 1), narrow_pick, BY_FIRST)

    copies = jnp.broadcast_to(packed, (lax.axis_size(ROW[:2]), *packed.shape))
    own_half = lax.all_to_all(copies, ROW[:2], 0, 0, tiled=True)
    own_half = own_half.reshape(width // 2, row_slots)
    other_half = lax.ppermute(own_half, ROW[2], [(0, 1), (1, 0)])
    lower = jnp.concatenate([own_half, other_half])

    narrow = dot(matrix, pick_cols).reshape(ratio, col_block, row_slots)
    dense = jnp.stack([dot(pick_rows[part], narrow[part], BY_FIRST) for part in range(ratio)])
    share = row_slots // col_count
    dense = jnp.moveaxis(dense.reshape(ratio, col_count, share, row_slots), 0, 1)
    dense = dense.reshape(ratio * row_slots, row_slots)

    partial_value = -dot(dense, lower, BY_LAST)
    summed = sum_at_owner(partial_value.reshape(col_count, ratio * share, width), COL)

    wide = ratio * row_k
    half_slots = col_slots // 2
    slots = col_count * col_slots
    found = panel_places(
        col_slots, col_block, ratio, col_count, factor.shape[1], panel_cols, row_lists
    )
    slot, local_slot = found[0], found[1]

    def route(places):
        return one_hot(places.reshape(-1), row_count * wide, jnp.bfloat16)

    to_rows = route(found[2:4])
    to_cols = route(found[4:6])

    halves_beside = jnp.concatenate([summed[:share], summed[share:]], axis=1)
    parts = thirds(halves_beside, 0)
    chosen = selected(parts, to_rows).reshape(share, row_count, wide)
    received = lax.all_to_all(jnp.moveaxis(chosen, 1, 0), ROW, 0, 0, tiled=True)

    own = jnp.moveaxis(selected(parts, to_cols).reshape(share, row_count, wide), 1, 0)
    lane = jnp.arange(wide, dtype=jnp.int32) // row_k
    sent = jnp.stack([jnp.where(lane == part, received, own) for part in range(ratio)], axis=1)
    arrived = lax.all_to_all(
        sent.reshape(col_count, share, wide), COL, 0, 0, tiled=True
    )
    arrived = arrived.reshape(row_slots, wide).T
    upper, under = arrived[:row_k], arrived[row_k:]
    beside = jnp.where(side == 0, upper, under)
    below = jnp.where(side == 0, under, upper)

    def halves(values):
        blocks = values.reshape(col_count, 2, half_slots, values.shape[1])
        return [blocks[:, part].reshape(col_count * half_slots, -1) for part in range(2)]

    lower_slots = dot(one_hot(local_slot, slots), lower, BY_FIRST)
    mine = lax.dynamic_slice_in_dim(slot, col_pos * dinv_rows, dinv_rows)
    placed = dot(
        one_hot(mine, slots), dot(dinv, one_hot(slot - row_pos * row_k, row_k)), BY_FIRST
    )
    lower_pair = jnp.concatenate(halves(lower_slots), axis=1)
    placed_pair = jnp.concatenate(halves(placed), axis=1)
    empty = jnp.zeros_like(beside)
    beside_pair = jnp.concatenate(
        [jnp.concatenate([beside, empty], axis=1), jnp.concatenate([empty, beside], axis=1)]
    )
    terms = placed_pair - dot(lower_pair, beside_pair, BY_LAST)
    corner = sum_at_owner(terms.reshape(col_count, half_slots, 2 * row_k), COL)

    below_rows = [dot(pick_rows[part], below[part * col_slots : (part + 1) * col_slots], BY_LAST) for part in range(ratio)]
    spread_out = dot(beside, pick_cols, BY_LAST)
    at_rows = jnp.concatenate(
        [
            dot(put_rows[part], spread_out[part * col_slots : (part + 1) * col_slots])
            for part in range(ratio)
        ]
    )
    with_rows = jnp.where(row_panel[:, None] & col_in[None, :], at_rows, matrix)
    corner = jnp.concatenate([corner[:, :row_k], corner[:, row_k:]])
    at_cols = jnp.concatenate(
        [
            below_rows[part]
            + dot(
                put_rows[part],
                corner[:, part * col_slots : (part + 1) * col_slots],
                BY_LAST,
            )
            for part in range(ratio)
        ]
    )
    thrice = jnp.concatenate([one_hot(panel_slot[:col_block], col_slots, jnp.bfloat16)] * 3, axis=1)
    at_cols = lax.dot_general(
        thirds(at_cols, 1),
        thrice,
        (BY_LAST, ((), ())),
        preferred_element_type=jnp.float32,
    )
    taken_over = (row_panel | row_in)[:, None] & col_panel[None, :]
    result = jnp.where(taken_over, at_cols, with_rows)

    fits = (jnp.max(found[6]) < col_slots) & (jnp.max(found[7]) <= row_slots)

    def again(carried):
        general = general_panel(matrix, factor, dinv, panel_cols, row_in, col_in)
        return jnp.zeros((), jnp.bool_), general

    return lax.while_loop(lambda carried: carried[0], again, (~fits, result))[1]


def on_device(resident, factor, dinv, panel_cols, row_lists):
    matrix = resident
    for panel in reversed(range(factor.shape[0])):
        matrix = panel_step(matrix, factor[panel], dinv[panel], panel_cols[panel], row_lists[panel])
    return matrix


def solution(mesh):
    finer = Mesh(
        mesh.devices.reshape(-1, 2, 2, mesh.shape["col"] // 2, 2), ROW + COL
    )
    return jax.shard_map(
        on_device,
        mesh=finer,
        in_specs=(P(ROW, COL), P(None, COL, ROW), P(None, COL, None), P(), P()),
        out_specs=P(ROW, COL),
        check_vma=False,
    )
```
